1024 devices in a mesh: grp: 4 (over x), dom: 16 (over z_lo, core), pen: 16 (over z_hi, y).
Axes of the slice: x: 4, y: 8, z: 16 (z_hi: 2, z_lo: 8; z = z_hi * 8 + z_lo), core: 2. Of those that a mesh axis runs over, the one named last changes fastest.
Arguments:
- atoms: float32 [4, 4, 16, 65536], P(None, 'grp', 'dom', 'pen'), may hold values from -6 to 6, as said below
- pair_home: int32 [4, 16, 1024], P('grp', 'dom', 'pen'), may hold values from 0 to 31
- pair_other: int32 [4, 16, 1024], P('grp', 'dom', 'pen'), may hold values from 0 to 287
Outputs:
- short_forces: float32 [3, 4, 16, 65536], P(None, 'grp', 'dom', 'pen')
- long_forces: float32 [3, 4, 16, 65536], P(None, 'grp', 'dom', 'pen')
The draws below stay inside these ranges and needn't reach their ends.
Inputs may be any that keep to these rules, and one draw needn't show every extreme that they name: `atoms`: in block (g, d, p) the first coordinate lies in [d / 16, (d + 0.98) / 16), the second in [p / 16, (p + 0.98) / 16), the third in [0, 1); the fourth component is the charge, within -6 to 6.
All inputs are finite; a program needn't handle non-finite values.
Results may differ from the reference program's by a relative error of at most 0.0003.
Values sent between devices are 32-bit elements; how exact they have to be, the bound alone decides.
A program may use at most 32 MiB of HBM per device.

```python
import math
import jax
import jax.numpy as jnp
from jax import lax

NG = 128
TILE = 128
A_DEV = 4096
PAIRS_DEV = 64
N_GRP = 4
N_DOM = 16
N_PEN = 16


def draw_atoms(key, part):
    subkeys = jax.random.split(jax.random.fold_in(key, 11), 4)
    shape = (N_GRP, N_DOM, N_PEN, A_DEV)
    dom_ids = lax.broadcasted_iota(jnp.float32, shape, 1)
    pen_ids = lax.broadcasted_iota(jnp.float32, shape, 2)
    coord_x = (dom_ids + 0.98 * jax.random.uniform(subkeys[0], shape, jnp.float32)) / N_DOM
    coord_y = (pen_ids + 0.98 * jax.random.uniform(subkeys[1], shape, jnp.float32)) / N_PEN
    coord_z = 0.999 * jax.random.uniform(subkeys[2], shape, jnp.float32)
    charge = jnp.clip(jax.random.normal(subkeys[3], shape, jnp.float32), -4.0, 4.0)
    stacked = jnp.stack([coord_x, coord_y, coord_z, charge])
    return stacked.reshape(4, N_GRP, N_DOM, N_PEN * A_DEV)


def place_ends(values, own_key, least, top_value):
    spot = [jax.random.randint(jax.random.fold_in(own_key, axis), (), 0, length) for axis, length in enumerate(values.shape)]
    widest = values.shape.index(max(values.shape))
    beside = spot[:widest] + [(spot[widest] + 1) % values.shape[widest]] + spot[widest + 1:]
    return values.at[tuple(spot)].set(least).at[tuple(beside)].set(top_value)


def setup_inputs(seed: int = 0) -> dict:
    key_list = jax.random.split(jax.random.key(seed), 4)
    atoms = draw_atoms(jax.random.fold_in(key_list[3], 71), 0)
    pair_home = place_ends(jax.random.randint(key_list[1], (N_GRP, N_DOM, N_PEN * PAIRS_DEV), 0, A_DEV // TILE), jax.random.fold_in(key_list[1], 1), 0, (A_DEV // TILE) - 1).astype(jnp.int32)
    pair_other = place_ends(jax.random.randint(key_list[2], (N_GRP, N_DOM, N_PEN * PAIRS_DEV), 0, 9 * (A_DEV // TILE)), jax.random.fold_in(key_list[2], 1), 0, (9 * (A_DEV // TILE)) - 1).astype(jnp.int32)
    return {"atoms": atoms, "pair_home": pair_home, "pair_other": pair_other}


def spline_terms(scaled):
    floored = jnp.floor(scaled)
    fraction = scaled - floored
    remain = 1.0 - fraction
    frac_sq = fraction * fraction
    frac_cube = frac_sq * fraction
    thetas = [remain * remain * remain / 6.0, (3.0 * frac_cube - 6.0 * frac_sq + 4.0) / 6.0, (-3.0 * frac_cube + 3.0 * frac_sq + 3.0 * fraction + 1.0) / 6.0, frac_cube / 6.0]
    slopes = [-0.5 * remain * remain, 1.5 * frac_sq - 2.0 * fraction, -1.5 * frac_sq + fraction + 0.5, 0.5 * frac_sq]
    return (floored.astype(jnp.int32) - 3, thetas, slopes)

def pair_push(home_pos, other_pos, scales):
    displace = home_pos[:, :3, :, None] - other_pos[:, :3, None, :]
    displace = displace - jnp.floor(displace + 0.5)
    scaled = displace * scales[None, :, None, None]
    weight = jnp.exp(-0.5 * lax.optimization_barrier(jnp.sum(scaled * scaled, axis=1))) * other_pos[:, 3, None, :]
    return lax.optimization_barrier(jnp.sum(scaled * weight[:, None], axis=3)) * home_pos[:, 3:4, :]

def green_factor(freq_x, freq_y, freq_z, grid_cells):

    def signed(frequencies):
        return jnp.where(frequencies < grid_cells // 2, frequencies, frequencies - grid_cells)

    def modulus(frequencies):
        turned = 2.0 * jnp.pi * signed(frequencies).astype(jnp.float32) / grid_cells
        ratio = (2.0 + jnp.cos(turned)) / 3.0
        return 1.0 / (ratio * ratio)
    signed_x = signed(freq_x)
    signed_y = signed(freq_y)
    signed_z = signed(freq_z)
    square = (signed_x * signed_x + signed_y * signed_y + signed_z * signed_z).astype(jnp.float32)
    beta = 0.6 * grid_cells
    safe = jnp.maximum(square, 1.0)
    value = jnp.exp(-jnp.pi * jnp.pi * square / (beta * beta)) / (jnp.pi * safe)
    value = value * modulus(freq_x) * modulus(freq_y) * modulus(freq_z)
    return jnp.where(square > 0.5, value, 0.0)

def reference(atoms, pair_home, pair_other):
    grid_cells = NG
    tile_count = A_DEV // TILE
    blocks = atoms.reshape(4, N_GRP, N_DOM, N_PEN, A_DEV)
    shifted = []
    for step_dom in (1, 0, -1):
        for step_pen in (1, 0, -1):
            shifted.append(jnp.roll(jnp.roll(blocks, step_dom, axis=2), step_pen, axis=3))
    nearby = jnp.stack(shifted).transpose(2, 3, 4, 0, 1, 5).reshape(N_GRP * N_DOM * N_PEN, 9, 4, A_DEV)
    homes = pair_home.reshape(-1, PAIRS_DEV)
    others = pair_other.reshape(-1, PAIRS_DEV)
    scales = jnp.array([2.0 * N_DOM, 2.0 * N_PEN, 2.0 * N_DOM], jnp.float32)

    def one_block(inputs):
        around, home_ids, other_ids = inputs
        tiled = around.reshape(9, 4, tile_count, TILE).transpose(0, 2, 1, 3).reshape(9 * tile_count, 4, TILE)
        own_tiles = tiled[4 * tile_count:5 * tile_count]
        pushes = pair_push(own_tiles[home_ids], tiled[other_ids], scales)
        totals = jnp.zeros((tile_count, 3, TILE), pushes.dtype).at[home_ids].add(pushes)
        return totals.transpose(1, 0, 2).reshape(3, A_DEV)
    short_out = lax.map(one_block, (nearby, homes, others))
    short_out = short_out.transpose(1, 0, 2).reshape(3, N_GRP, N_DOM, N_PEN * A_DEV)
    short_out = short_out * (2.0 / math.sqrt(A_DEV / N_DOM))
    flat = atoms.reshape(4, -1)
    charge = flat[3]
    terms = [spline_terms(flat[axis_id] * grid_cells) for axis_id in range(3)]
    corner = jnp.arange(4, dtype=jnp.int32)
    z_ids = jnp.mod(terms[2][0][:, None] + corner[None, :], grid_cells)
    z_weights = jnp.stack(terms[2][1], axis=1)
    z_slopes = jnp.stack(terms[2][2], axis=1)
    charge_mesh = jnp.zeros((grid_cells, grid_cells, grid_cells), flat.dtype)
    for step_x in range(4):
        x_ids = jnp.mod(terms[0][0] + step_x, grid_cells)
        for step_y in range(4):
            y_ids = jnp.mod(terms[1][0] + step_y, grid_cells)
            amount = (charge * terms[0][1][step_x] * terms[1][1][step_y])[:, None] * z_weights
            charge_mesh = charge_mesh.at[x_ids[:, None], y_ids[:, None], z_ids].add(amount)
    frequencies = jnp.arange(grid_cells, dtype=jnp.int32)
    green = green_factor(frequencies[:, None, None], frequencies[None, :, None], frequencies[None, None, :], grid_cells)
    potential = jnp.real(jnp.fft.ifftn(jnp.fft.fftn(charge_mesh) * green)) * float(grid_cells) ** 3
    grads = [jnp.zeros_like(charge) for axis_id in range(3)]
    for step_x in range(4):
        x_ids = jnp.mod(terms[0][0] + step_x, grid_cells)
        for step_y in range(4):
            y_ids = jnp.mod(terms[1][0] + step_y, grid_cells)
            picked = potential[x_ids[:, None], y_ids[:, None], z_ids]
            along_z = lax.optimization_barrier(jnp.sum(picked * z_weights, axis=1))
            slope_z = lax.optimization_barrier(jnp.sum(picked * z_slopes, axis=1))
            grads[0] = grads[0] + terms[0][2][step_x] * terms[1][1][step_y] * along_z
            grads[1] = grads[1] + terms[0][1][step_x] * terms[1][2][step_y] * along_z
            grads[2] = grads[2] + terms[0][1][step_x] * terms[1][1][step_y] * slope_z
    total_atoms = A_DEV * N_GRP * N_DOM * N_PEN
    long_scale = -0.4 * grid_cells / math.sqrt(grid_cells * total_atoms)
    long_out = (jnp.stack(grads) * charge[None, :] * long_scale).reshape(3, N_GRP, N_DOM, N_PEN * A_DEV)
    return (short_out, long_out)
```

```python
import functools
import math

import jax
import jax.numpy as jnp
import numpy as np
from jax import lax
from jax.experimental import pallas as pl
from jax.experimental.pallas import tpu as pltpu
from jax.sharding import PartitionSpec as P

NG = 128
TILE = 128
TILES = 32
PAIRS = 64
SIDE = 11
PEERS = 32
MESH = pl.DeviceIdType.MESH
f32 = jnp.float32
bf16 = jnp.bfloat16


def basis(cells):
    k = np.arange(NG)[:, None]
    m = np.where(k <= NG // 2, k, k - NG // 2)
    angle = 2.0 * np.pi * np.mod(m * cells[None, :], NG) / NG
    return np.where(k <= NG // 2, np.cos(angle), np.sin(angle))


def turning(starts, lanes, used):
    k = np.arange(NG)[:, None]
    m = np.where(k <= NG // 2, k, k - NG // 2)
    first = 2.0 * np.pi * np.mod(m * starts[None, :], NG) / NG
    second = 2.0 * np.pi * np.mod(m * lanes[None, :], NG) / NG
    is_cos = k <= NG // 2
    part_c = np.where(is_cos, np.cos(second), np.sin(second)) * used[None, :]
    part_s = np.where(is_cos, -np.sin(second), np.cos(second)) * used[None, :]
    return np.cos(first), np.sin(first), part_c, part_s


def halves(table):
    table = np.asarray(table, np.float32)
    high = table.astype(jnp.bfloat16)
    low = (table - high.astype(np.float32)).astype(jnp.bfloat16)
    return high, low


def spread_columns(turn_c, turn_s, inner):
    count = turn_c.shape[1]
    out = np.zeros((inner, 2, NG, count, inner))
    for i in range(inner):
        out[i, 0, :, :, i] = turn_c
        out[i, 1, :, :, i] = turn_s
    return out.reshape(inner * 2 * NG, count * inner)


def make_tables():
    row = np.arange(NG)
    row_x, row_y = row // SIDE, row % SIDE
    lane_z, lane_y = (row // 16) % 2, row % 16
    x_c, x_s, bx_c, bx_s = turning(8 * np.arange(16), row_x - 3, row < SIDE * SIDE)
    y_c, y_s, by_c, by_s = turning(8 * np.arange(8), 64 * lane_z - 3 + lane_y, lane_y < SIDE)
    x_cols, y_cols = spread_columns(x_c, x_s, 4), spread_columns(y_c, y_s, 4)
    xh, xl = halves(x_cols)
    yh, yl = halves(y_cols)
    forward_x = np.concatenate([xh, xh, xl], axis=1)
    forward_y = np.concatenate([yh, yh, yl], axis=1)
    inverse_x = np.concatenate([xh.T, xl.T], axis=0)
    inverse_y = np.concatenate([yh.T, yl.T], axis=0)
    pick_x = np.zeros((4, 2, NG, NG), np.float32)
    for j in range(4):
        for z in range(2):
            for r in range(SIDE * SIDE):
                pick_x[j, z, r, j * 32 + z * 16 + row_y[r]] = 1.0
    pick_y = np.zeros((4, NG, NG), np.float32)
    for i in range(4):
        for lane in range(NG):
            pick_y[i, lane, i * 4 + lane // 32] = 1.0
    zh, zl = halves(basis(row))
    return dict(
        basis_z=np.concatenate([zh, zl], axis=0),
        forward_x=forward_x,
        forward_y=forward_y,
        inverse_x=inverse_x,
        inverse_y=inverse_y,
        pick_x=pick_x.reshape(1024, NG).astype(jnp.bfloat16),
        pick_y=pick_y.reshape(512, NG).astype(jnp.bfloat16),
        parts=np.concatenate([bx_c, bx_s, by_c, by_s], axis=0).astype(np.float32),
    )


NAMES = (
    "basis_z",
    "forward_x",
    "forward_y",
    "inverse_x",
    "inverse_y",
    "pick_x",
    "pick_y",
    "parts",
)


def dot(a, b):
    return lax.dot_general(a, b, (((1,), (0,)), ((), ())), preferred_element_type=f32)


def dot_nt(a, b):
    return lax.dot_general(a, b, (((1,), (1,)), ((), ())), preferred_element_type=f32)


def split(x):
    high = x.astype(bf16)
    return high, (x - high.astype(f32)).astype(bf16)


def stacked(x):
    high = x.astype(bf16).astype(f32)
    return jnp.concatenate([high, x - high, high], axis=0).astype(bf16)


def spline_terms(scaled):
    floored = jnp.floor(scaled)
    w = scaled - floored
    remain = 1.0 - w
    sq = w * w
    cube = sq * w
    thetas = [
        remain * remain * remain * (1.0 / 6.0),
        (3.0 * cube - 6.0 * sq + 4.0) * (1.0 / 6.0),
        (-3.0 * cube + 3.0 * sq + 3.0 * w + 1.0) * (1.0 / 6.0),
        cube * (1.0 / 6.0),
    ]
    slopes = [
        -0.5 * remain * remain,
        1.5 * sq - 2.0 * w,
        -1.5 * sq + w + 0.5,
        0.5 * sq,
    ]
    return floored, thetas, slopes


def one_of(is_at, values):
    out = jnp.where(is_at[3], values[3], 0.0)
    for k in (2, 1, 0):
        out = jnp.where(is_at[k], values[k], out)
    return out


def matches(t):
    return [t == k for k in range(4)]


def to_lines_x(got, forward_x, part_c, part_s, pick_x):
    both = jnp.concatenate([got[:64], got[64:]], axis=1)
    turned = dot(forward_x, stacked(both))
    c2, s2 = jnp.concatenate([part_c] * 2, axis=1), jnp.concatenate([part_s] * 2, axis=1)
    out = None
    for j in range(4):
        q = c2 * turned[j * 256 : j * 256 + 128] + s2 * turned[j * 256 + 128 : j * 256 + 256]
        high, low = split(q)
        pick = pick_x[j * 256 : (j + 1) * 256]
        term = dot(high, pick) + dot(low, pick)
        out = term if out is None else out + term
    return out


def through_y(got, factor, forward_y, inverse_y, part_c, part_s, pick_y):
    total = (got[:32] + got[32:64]) + (got[64:96] + got[96:])
    turned = dot(forward_y, stacked(total))
    lines = jnp.concatenate(
        [
            part_c * turned[i * 256 : i * 256 + 128] + part_s * turned[i * 256 + 128 : i * 256 + 256]
            for i in range(4)
        ],
        axis=1,
    )
    high, low = split(lines)
    freq = (dot(high, pick_y) + dot(low, pick_y)) * factor
    high, low = split(freq)
    wide = dot_nt(high, pick_y) + dot_nt(low, pick_y)
    out = None
    for i in range(4):
        piece = wide[:, i * 128 : (i + 1) * 128]
        high, low = split(jnp.concatenate([part_c * piece, part_s * piece], axis=0))
        table = inverse_y[:, i * 256 : (i + 1) * 256]
        full = dot(table, high)
        term = full[:32] + full[32:] + dot(table[:32], low)
        out = term if out is None else out + term
    return out


def from_lines_x(got, inverse_x, part_c, part_s, pick_x):
    high, low = split(got)
    c2, s2 = jnp.concatenate([part_c] * 2, axis=1), jnp.concatenate([part_s] * 2, axis=1)
    out = None
    for j in range(4):
        pick = pick_x[j * 256 : (j + 1) * 256]
        wide = dot_nt(high, pick) + dot_nt(low, pick)
        q_high, q_low = split(jnp.concatenate([c2 * wide, s2 * wide], axis=0))
        table = inverse_x[:, j * 256 : (j + 1) * 256]
        full = dot(table, q_high)
        term = full[:64] + full[64:] + dot(table[:64], q_low)
        out = term if out is None else out + term
    return jnp.concatenate([out[:, :128], out[:, 128:]], axis=0)


def to_z(mesh, basis_z):
    high, low = split(mesh)
    full = dot(basis_z, high)
    return full[:128] + full[128:] + dot(basis_z[:128], low)


def from_z(got, basis_z):
    high, low = split(got.T)
    return dot(high, basis_z[:128]) + dot(high, basis_z[128:]) + dot(low, basis_z[:128])


def green_of(k_x, k_y, k_z):
    def mode(k):
        return jnp.where(k <= NG // 2, k, k - NG // 2)

    def weight(m):
        ratio = (2.0 + jnp.cos(m.astype(f32) * (2.0 * math.pi / NG))) / 3.0
        twice = jnp.where((m == 0) | (m == NG // 2), 1.0, 2.0)
        return twice / (ratio * ratio)

    m_x, m_y, m_z = mode(k_x), mode(k_y), mode(k_z)
    square = (m_x * m_x + m_z * m_z + m_y * m_y).astype(f32)
    beta = 0.6 * NG
    value = jnp.exp(square * (-math.pi * math.pi / (beta * beta)))
    value = value / (math.pi * jnp.maximum(square, 1.0))
    value = value * (weight(m_x) * weight(m_z)) * weight(m_y)
    return jnp.where(square > 0.5, value, 0.0)


def pair_push(home, other, scales):
    scaled = []
    for c in range(3):
        delta = home[c] - other[:, c : c + 1]
        delta = delta - jnp.floor(delta + 0.5)
        scaled.append(delta * scales[c])
    square = scaled[0] * scaled[0] + scaled[1] * scaled[1] + scaled[2] * scaled[2]
    weight = jnp.exp(-0.5 * square) * other[:, 3:4]
    return [jnp.sum(s * weight, axis=0, keepdims=True) for s in scaled]


LOW = 0
THETA = 3
SLOPE = 15
CHARGED = 27
FIELDS = 31


def kernel(
    atoms_hbm,
    home_smem,
    other_smem,
    home_vmem,
    basis_hbm,
    fx_hbm,
    fy_hbm,
    ix_hbm,
    iy_hbm,
    px_hbm,
    py_hbm,
    parts_hbm,
    short_ref,
    long_ref,
    near,
    fields,
    mesh,
    pushes,
    grads,
    pot_parts,
    send_a,
    recv_a,
    send_b,
    recv_b,
    send_c,
    recv_c,
    send_d,
    recv_d,
    basis_z,
    forward_x,
    forward_y,
    inverse_x,
    inverse_y,
    pick_x,
    pick_y,
    parts,
    table_sems,
    atom_sem,
    send_sems,
    recv_sems,
    halo_send,
    halo_recv,
):
    grp = lax.axis_index("grp")
    dom = lax.axis_index("dom")
    pen = lax.axis_index("pen")
    z_hi, y_at = pen // 8, lax.rem(pen, 8)
    at_a = z_hi * 16 + dom
    at_b = grp * 8 + y_at

    def peer_a(k):
        t = lax.rem(at_a + k, PEERS)
        return t, {"grp": grp, "dom": lax.rem(t, 16), "pen": (t // 16) * 8 + y_at}

    def peer_b(k):
        b = lax.rem(at_b + k, PEERS)
        return b, {"grp": b // 8, "dom": dom, "pen": z_hi * 8 + lax.rem(b, 8)}

    pen_next = {"grp": grp, "dom": dom, "pen": lax.rem(pen + 1, 16)}
    pen_prev = {"grp": grp, "dom": dom, "pen": lax.rem(pen + 15, 16)}
    dom_next = {"grp": grp, "dom": lax.rem(dom + 1, 16), "pen": pen}
    dom_prev = {"grp": grp, "dom": lax.rem(dom + 15, 16), "pen": pen}

    load_atoms = pltpu.make_async_copy(atoms_hbm, near.at[4], atom_sem)
    load_atoms.start()
    barrier = pltpu.get_barrier_semaphore()

    def greet(k, carry):
        pl.semaphore_signal(barrier, 1, device_id=peer_a(k)[1], device_id_type=MESH)
        pl.semaphore_signal(barrier, 1, device_id=peer_b(k)[1], device_id_type=MESH)
        return carry

    lax.fori_loop(1, PEERS, greet, 0)
    pl.semaphore_signal(barrier, 1, device_id=pen_next, device_id_type=MESH)
    pl.semaphore_signal(barrier, 1, device_id=pen_prev, device_id_type=MESH)

    loads = [
        pltpu.make_async_copy(source, target, table_sems.at[n])
        for n, (source, target) in enumerate(
            (
                (basis_hbm, basis_z),
                (fx_hbm, forward_x),
                (fy_hbm, forward_y),
                (ix_hbm, inverse_x),
                (iy_hbm, inverse_y),
                (px_hbm, pick_x),
                (py_hbm, pick_y),
                (parts_hbm, parts),
            )
        )
    ]
    for load in loads:
        load.start()
    load_atoms.wait()

    charge = near[4, 3]
    for c, start in ((0, (dom * 8).astype(f32)), (1, (pen * 8).astype(f32)), (2, 3.0)):
        floored, thetas, slopes = spline_terms(near[4, c] * float(NG))
        fields[LOW + c] = floored - start
        for k in range(4):
            fields[THETA + 4 * c + k] = thetas[k]
            fields[SLOPE + 4 * c + k] = slopes[k]
            if c == 1:
                fields[CHARGED + k] = thetas[k] * charge

    column = lax.broadcasted_iota(jnp.int32, (NG, TILE), 0)
    patch_x = jnp.floor((column.astype(f32) + 0.5) * (1.0 / SIDE))
    patch_y = column.astype(f32) - SIDE * patch_x

    def row(field, tile):
        return fields[field, pl.ds(tile, 1), :]

    def at_z(tile):
        return matches((column - row(LOW + 2, tile).astype(jnp.int32)) & (NG - 1))

    mesh[...] = jnp.zeros_like(mesh)

    def spread(step, carry):
        z_parts, p_parts = [], []
        for n in range(4):
            tile = step * 4 + n
            w_z = one_of(at_z(tile), [row(THETA + 8 + k, tile) for k in range(4)])
            w_x = one_of(
                matches(patch_x - row(LOW, tile)), [row(THETA + k, tile) for k in range(4)]
            )
            w_y = one_of(
                matches(patch_y - row(LOW + 1, tile)), [row(CHARGED + k, tile) for k in range(4)]
            )
            z_parts.append(split(w_z))
            p_parts.append(split(w_x * w_y))
        z_high = jnp.concatenate([z[0] for z in z_parts], axis=1)
        z_low = jnp.concatenate([z[1] for z in z_parts], axis=1)
        p_high = jnp.concatenate([p[0] for p in p_parts], axis=1)
        p_low = jnp.concatenate([p[1] for p in p_parts], axis=1)
        wide = dot_nt(z_high, jnp.concatenate([p_high, p_low], axis=0))
        mesh[...] += wide[:, :128] + wide[:, 128:] + dot_nt(z_low, p_high)
        return carry

    lax.fori_loop(0, TILES // 4, spread, 0)

    def put(ref, value):
        for n in range(value.shape[0] // 4):
            ref[n] = value[4 * n : 4 * n + 4]

    def taken(ref):
        return jnp.concatenate([ref[n] for n in range(PEERS)], axis=0)

    def exchange(source, target, phase, peer, own, slot):
        def post(k, carry):
            index, device = peer(k)
            pltpu.make_async_remote_copy(
                src_ref=source.at[slot(index)],
                dst_ref=target.at[own],
                send_sem=send_sems.at[phase],
                recv_sem=recv_sems.at[phase],
                device_id=device,
                device_id_type=MESH,
            ).start()
            return carry

        lax.fori_loop(1, PEERS, post, 0)
        target[own] = source[slot(own)]

    def arrived(target, phase, device):
        whole = target.at[pl.ds(0, PEERS - 1)]
        both = pltpu.make_async_remote_copy(
            src_ref=whole,
            dst_ref=whole,
            send_sem=send_sems.at[phase],
            recv_sem=recv_sems.at[phase],
            device_id=device,
            device_id_type=MESH,
        )
        both.wait_recv()
        both.wait_send()

    def same(index):
        return index

    loads[0].wait()
    put(send_a, to_z(mesh[...], basis_z[...]))
    pl.semaphore_wait(barrier, 2 * (PEERS - 1) + 2)
    exchange(send_a, recv_a, 0, peer_a, at_a, same)

    def halo(source, target, n, device):
        return pltpu.make_async_remote_copy(
            src_ref=near.at[source],
            dst_ref=near.at[target],
            send_sem=halo_send.at[n],
            recv_sem=halo_recv.at[n],
            device_id=device,
            device_id_type=MESH,
        )

    side = [halo(4, 3, 0, pen_next), halo(4, 5, 1, pen_prev)]
    for copy in side:
        copy.start()

    for load in loads[1:]:
        load.wait()
    part_xc, part_xs, part_yc, part_ys = (parts[128 * n : 128 * n + 128, :] for n in range(4))
    lane = lax.broadcasted_iota(jnp.int32, (1, NG), 1)
    k_x = at_b * 4 + (lane // 4)
    k_z = at_a * 4 + lax.rem(lane, 4)
    k_y = lax.broadcasted_iota(jnp.int32, (NG, 1), 0)
    used = lane < 16
    factor = green_of(jnp.where(used, k_x, 1), k_y, jnp.where(used, k_z, 1))

    peer_one_a = peer_a(1)[1]
    peer_one_b = peer_b(1)[1]
    arrived(recv_a, 0, peer_one_a)
    put(send_b, to_lines_x(taken(recv_a), forward_x[...], part_xc, part_xs, pick_x[...]))
    exchange(send_b, recv_b, 1, peer_b, at_b, same)

    arrived(recv_b, 1, peer_one_b)
    put(
        send_c,
        through_y(
            taken(recv_b),
            factor,
            forward_y[...],
            inverse_y[...],
            part_yc,
            part_ys,
            pick_y[...],
        ),
    )
    exchange(send_c, recv_c, 2, peer_b, at_b, lambda index: lax.rem(index, 8))

    for copy in side:
        copy.wait()
    ends = [
        halo(pl.ds(3, 3), pl.ds(0, 3), 2, dom_next),
        halo(pl.ds(3, 3), pl.ds(6, 3), 3, dom_prev),
    ]
    for copy in ends:
        copy.start()

    arrived(recv_c, 2, peer_one_b)
    put(send_d, from_lines_x(taken(recv_c), inverse_x[...], part_xc, part_xs, pick_x[...]))
    exchange(send_d, recv_d, 3, peer_a, at_a, same)

    for copy in ends:
        copy.wait()
    scales = (32.0, 32.0, 32.0)
    pad = jnp.zeros((4, TILE), f32)

    def pair(n, carry):
        home, other = home_smem[n], other_smem[n]
        own = [near[4, c, pl.ds(home, 1), :] for c in range(3)]
        far = [near[other >> 5, c, pl.ds(other & 31, 1), :] for c in range(4)]
        rows = pair_push(own, jnp.concatenate(far + [pad], axis=0).T, scales)
        for c in range(3):
            pushes[c, pl.ds(n, 1), :] = rows[c]
        return carry

    lax.fori_loop(0, PAIRS, pair, 0, unroll=2)
    tile_ids = lax.broadcasted_iota(jnp.int32, (TILES, PAIRS), 0)
    owners = jnp.where(home_vmem[...] == tile_ids, 1.0, 0.0).astype(bf16)
    for c in range(3):
        high, low = split(pushes[c])
        short_ref[c] = (dot(owners, high) + dot(owners, low)) * (charge * (2.0 / math.sqrt(256.0)))

    arrived(recv_d, 3, peer_one_a)
    pot_high, pot_low = split(from_z(taken(recv_d), basis_z[...]))
    pot_parts[:128] = pot_high
    pot_parts[128:] = pot_low

    def interpolate(step, carry):
        for n in range(2):
            tile = step * 2 + n
            is_z = at_z(tile)
            w_z = one_of(is_z, [row(THETA + 8 + k, tile) for k in range(4)])
            s_z = one_of(is_z, [row(SLOPE + 8 + k, tile) for k in range(4)])
            high, low = split(jnp.concatenate([w_z, s_z], axis=1))
            full = dot(pot_parts[...], high)
            along = full[:128] + full[128:] + dot(pot_parts[:128], low)
            is_x = matches(patch_x - row(LOW, tile))
            w_x = one_of(is_x, [row(THETA + k, tile) for k in range(4)])
            s_x = one_of(is_x, [row(SLOPE + k, tile) for k in range(4)])
            is_y = matches(patch_y - row(LOW + 1, tile))
            w_y = one_of(is_y, [row(THETA + 4 + k, tile) for k in range(4)])
            s_y = one_of(is_y, [row(SLOPE + 4 + k, tile) for k in range(4)])
            value, slope = along[:, :128], along[:, 128:]
            sums = (s_x * (w_y * value), w_x * (s_y * value), w_x * (w_y * slope))
            for c in range(3):
                grads[c, pl.ds(tile, 1), :] = jnp.sum(sums[c], axis=0, keepdims=True)
        return carry

    lax.fori_loop(0, TILES // 2, interpolate, 0)
    total_atoms = 4 * 16 * 16 * 4096
    scale = -0.4 * NG / math.sqrt(NG * total_atoms)
    for c in range(3):
        long_ref[c] = grads[c] * (charge * scale)


def on_device(atoms, pair_home, pair_other, *tables):
    any_spec = pl.BlockSpec(memory_space=pl.ANY)
    smem = pl.BlockSpec(memory_space=pltpu.SMEM)
    vmem = pl.BlockSpec(memory_space=pltpu.VMEM)
    blocks = atoms.reshape(4, TILES, TILE)
    homes = pair_home.reshape(PAIRS)
    others = pair_other.reshape(PAIRS)
    force = jax.ShapeDtypeStruct((3, TILES, TILE), f32)
    message = pltpu.VMEM((PEERS, 4, NG), f32)
    short, long = pl.pallas_call(
        kernel,
        out_shape=(force, force),
        in_specs=[any_spec, smem, smem, vmem] + [any_spec] * len(NAMES),
        out_specs=(vmem, vmem),
        scratch_shapes=[
            pltpu.VMEM((9, 4, TILES, TILE), f32),
            pltpu.VMEM((FIELDS, TILES, TILE), f32),
            pltpu.VMEM((NG, NG), f32),
            pltpu.VMEM((3, PAIRS, TILE), f32),
            pltpu.VMEM((3, TILES, TILE), f32),
            pltpu.VMEM((2 * NG, NG), bf16),
            message,
            message,
            message,
            message,
            pltpu.VMEM((8, 4, NG), f32),
            message,
            message,
            message,
            *[pltpu.VMEM(t.shape, t.dtype) for t in tables],
            pltpu.SemaphoreType.DMA((len(NAMES),)),
            pltpu.SemaphoreType.DMA,
            pltpu.SemaphoreType.DMA((4,)),
            pltpu.SemaphoreType.DMA((4,)),
            pltpu.SemaphoreType.DMA((4,)),
            pltpu.SemaphoreType.DMA((4,)),
        ],
        compiler_params=pltpu.CompilerParams(
            collective_id=0, has_side_effects=True, vmem_limit_bytes=48 << 20
        ),
        name="forces",
    )(blocks, homes, others, homes.reshape(1, PAIRS), *tables)
    return short.reshape(3, 1, 1, TILES * TILE), long.reshape(3, 1, 1, TILES * TILE)


def solution(mesh):
    tables = make_tables()

    def whole(atoms, pair_home, pair_other):
        fixed = [jnp.asarray(tables[name]) for name in NAMES]
        mapped = jax.shard_map(
            lambda a, h, o: on_device(a, h, o, *fixed),
            mesh=mesh,
            in_specs=(P(None, "grp", "dom", "pen"), P("grp", "dom", "pen"), P("grp", "dom", "pen")),
            out_specs=(P(None, "grp", "dom", "pen"), P(None, "grp", "dom", "pen")),
            check_vma=False,
        )
        return mapped(atoms, pair_home, pair_other)

    return whole
```

```python
import functools
import math

import jax
import jax.numpy as jnp
import numpy as np
from jax import lax
from jax.experimental import pallas as pl
from jax.experimental.pallas import tpu as pltpu
from jax.sharding import PartitionSpec as P

NG = 128
TILE = 128
TILES = 32
PAIRS = 64
SIDE = 11
PEERS = 32
MESH = pl.DeviceIdType.MESH
f32 = jnp.float32
bf16 = jnp.bfloat16


def basis(cells):
    k = np.arange(NG)[:, None]
    m = np.where(k <= NG // 2, k, k - NG // 2)
    angle = 2.0 * np.pi * np.mod(m * cells[None, :], NG) / NG
    return np.where(k <= NG // 2, np.cos(angle), np.sin(angle))


def turning(starts, lanes, used):
    k = np.arange(NG)[:, None]
    m = np.where(k <= NG // 2, k, k - NG // 2)
    first = 2.0 * np.pi * np.mod(m * starts[None, :], NG) / NG
    second = 2.0 * np.pi * np.mod(m * lanes[None, :], NG) / NG
    is_cos = k <= NG // 2
    part_c = np.where(is_cos, np.cos(second), np.sin(second)) * used[None, :]
    part_s = np.where(is_cos, -np.sin(second), np.cos(second)) * used[None, :]
    return np.cos(first), np.sin(first), part_c, part_s


def halves(table):
    table = np.asarray(table, np.float32)
    high = table.astype(jnp.bfloat16)
    low = (table - high.astype(np.float32)).astype(jnp.bfloat16)
    return high, low


def spread_columns(turn_c, turn_s, inner):
    count = turn_c.shape[1]
    out = np.zeros((inner, 2, NG, count, inner))
    for i in range(inner):
        out[i, 0, :, :, i] = turn_c
        out[i, 1, :, :, i] = turn_s
    return out.reshape(inner * 2 * NG, count * inner)


def patch_places():
    places = [(x, y) for y in range(SIDE) for x in range(8)]
    places += [(x, y) for x in range(8, SIDE) for y in range(8)]
    places += [(x, y) for x in range(8, SIDE) for y in range(8, SIDE)]
    places += [(SIDE, SIDE)] * (NG - len(places))
    return np.array(places).T


def make_tables():
    row = np.arange(NG)
    row_x, row_y = patch_places()
    lane_z, lane_y = (row // 16) % 2, row % 16
    x_c, x_s, bx_c, bx_s = turning(8 * np.arange(16), row_x - 3, row < SIDE * SIDE)
    y_c, y_s, by_c, by_s = turning(8 * np.arange(8), 64 * lane_z - 3 + lane_y, lane_y < SIDE)
    x_cols, y_cols = spread_columns(x_c, x_s, 4), spread_columns(y_c, y_s, 4)
    xh, xl = halves(x_cols)
    yh, yl = halves(y_cols)
    forward_x = np.concatenate([xh, xh, xl], axis=1)
    forward_y = np.concatenate([yh, yh, yl], axis=1)
    inverse_x = np.concatenate([xh.T, xl.T], axis=0)
    inverse_y = np.concatenate([yh.T, yl.T], axis=0)
    pick_x = np.zeros((4, 2, NG, NG), np.float32)
    for j in range(4):
        for z in range(2):
            for r in range(SIDE * SIDE):
                pick_x[j, z, r, j * 32 + z * 16 + row_y[r]] = 1.0
    pick_y = np.zeros((4, NG, NG), np.float32)
    for i in range(4):
        for lane in range(NG):
            pick_y[i, lane, i * 4 + lane // 32] = 1.0
    zh, zl = halves(basis(row))
    return dict(
        forward_x=forward_x,
        forward_y=forward_y,
        inverse=np.concatenate([inverse_x, inverse_y], axis=0),
        picks=np.concatenate(
            [
                pick_x.reshape(1024, NG).astype(jnp.bfloat16),
                pick_y.reshape(512, NG).astype(jnp.bfloat16),
                zh,
                zl,
            ],
            axis=0,
        ),
        parts=np.concatenate([bx_c, bx_s, by_c, by_s], axis=0).astype(np.float32),
    )


NAMES = (
    "picks",
    "forward_x",
    "forward_y",
    "inverse",
    "parts",
)


def dot(a, b):
    return lax.dot_general(a, b, (((1,), (0,)), ((), ())), preferred_element_type=f32)


def dot_nt(a, b):
    return lax.dot_general(a, b, (((1,), (1,)), ((), ())), preferred_element_type=f32)


def split(x):
    high = x.astype(bf16)
    return high, (x - high.astype(f32)).astype(bf16)


def stacked(x):
    high = x.astype(bf16).astype(f32)
    return jnp.concatenate([high, x - high, high], axis=0).astype(bf16)


def spline_terms(scaled):
    floored = jnp.floor(scaled)
    w = scaled - floored
    remain = 1.0 - w
    sq = w * w
    cube = sq * w
    thetas = [
        remain * remain * remain * (1.0 / 6.0),
        (3.0 * cube - 6.0 * sq + 4.0) * (1.0 / 6.0),
        (-3.0 * cube + 3.0 * sq + 3.0 * w + 1.0) * (1.0 / 6.0),
        cube * (1.0 / 6.0),
    ]
    slopes = [
        -0.5 * remain * remain,
        1.5 * sq - 2.0 * w,
        -1.5 * sq + w + 0.5,
        0.5 * sq,
    ]
    return floored, thetas, slopes


def one_of(is_at, values):
    out = jnp.where(is_at[3], values[3], 0.0)
    for k in (2, 1, 0):
        out = jnp.where(is_at[k], values[k], out)
    return out


def matches(t):
    return [t == k for k in range(4)]


def to_lines_x(got, forward_x, part_c, part_s, pick_x):
    both = jnp.concatenate([got[:64], got[64:]], axis=1)
    turned = dot(forward_x, stacked(both))
    c2, s2 = jnp.concatenate([part_c] * 2, axis=1), jnp.concatenate([part_s] * 2, axis=1)
    out = None
    for j in range(4):
        q = c2 * turned[j * 256 : j * 256 + 128] + s2 * turned[j * 256 + 128 : j * 256 + 256]
        high, low = split(q)
        pick = pick_x[j * 256 : (j + 1) * 256]
        term = dot(high, pick) + dot(low, pick)
        out = term if out is None else out + term
    return out


def through_y(got, factor, forward_y, inverse_y, part_c, part_s, pick_y):
    total = (got[:32] + got[32:64]) + (got[64:96] + got[96:])
    turned = dot(forward_y, stacked(total))
    lines = jnp.concatenate(
        [
            part_c * turned[i * 256 : i * 256 + 128] + part_s * turned[i * 256 + 128 : i * 256 + 256]
            for i in range(4)
        ],
        axis=1,
    )
    high, low = split(lines)
    freq = (dot(high, pick_y) + dot(low, pick_y)) * factor
    high, low = split(freq)
    wide = dot_nt(high, pick_y) + dot_nt(low, pick_y)
    out = None
    for i in range(4):
        piece = wide[:, i * 128 : (i + 1) * 128]
        high, low = split(jnp.concatenate([part_c * piece, part_s * piece], axis=0))
        table = inverse_y[:, i * 256 : (i + 1) * 256]
        full = dot(table, high)
        term = full[:32] + full[32:] + dot(table[:32], low)
        out = term if out is None else out + term
    return out


def from_lines_x(got, inverse_x, part_c, part_s, pick_x):
    high, low = split(got)
    c2, s2 = jnp.concatenate([part_c] * 2, axis=1), jnp.concatenate([part_s] * 2, axis=1)
    out = None
    for j in range(4):
        pick = pick_x[j * 256 : (j + 1) * 256]
        wide = dot_nt(high, pick) + dot_nt(low, pick)
        q_high, q_low = split(jnp.concatenate([c2 * wide, s2 * wide], axis=0))
        table = inverse_x[:, j * 256 : (j + 1) * 256]
        full = dot(table, q_high)
        term = full[:64] + full[64:] + dot(table[:64], q_low)
        out = term if out is None else out + term
    return jnp.concatenate([out[:, :128], out[:, 128:]], axis=0)


def to_z(mesh, basis_z):
    high, low = split(mesh)
    full = dot(basis_z, high)
    return full[:128] + full[128:] + dot(basis_z[:128], low)


def from_z(got, basis_z):
    high, low = split(got.T)
    return dot(high, basis_z[:128]) + dot(high, basis_z[128:]) + dot(low, basis_z[:128])


def green_of(k_x, k_y, k_z):
    def mode(k):
        return jnp.where(k <= NG // 2, k, k - NG // 2)

    def weight(m):
        ratio = (2.0 + jnp.cos(m.astype(f32) * (2.0 * math.pi / NG))) / 3.0
        twice = jnp.where((m == 0) | (m == NG // 2), 1.0, 2.0)
        return twice / (ratio * ratio)

    m_x, m_y, m_z = mode(k_x), mode(k_y), mode(k_z)
    square = (m_x * m_x + m_z * m_z + m_y * m_y).astype(f32)
    beta = 0.6 * NG
    value = jnp.exp(square * (-math.pi * math.pi / (beta * beta)))
    value = value / (math.pi * jnp.maximum(square, 1.0))
    value = value * (weight(m_x) * weight(m_z)) * weight(m_y)
    return jnp.where(square > 0.5, value, 0.0)


def thirds(x):
    high = x.astype(bf16).astype(f32)
    rest = x - high
    middle = rest.astype(bf16).astype(f32)
    return high, middle, rest - middle


def pair_push(other, against):
    columns = jnp.concatenate([*thirds(other), jnp.ones_like(other)], axis=0).astype(bf16)
    wide = lax.dot_general(
        columns, against, (((0,), (0,)), ((), ())), preferred_element_type=f32
    )
    delta = [wide[:, 128 * c : 128 * c + 128] for c in range(3)]
    delta[2] = delta[2] - jnp.floor(delta[2] + 0.5)
    square = delta[0] * delta[0] + delta[1] * delta[1] + delta[2] * delta[2]
    weight = jnp.exp2(square * (-512.0 * math.log2(math.e))) * wide[:, 384:]
    return [jnp.sum(d * weight, axis=0, keepdims=True) for d in delta]


PLACE = 0
THETA = 12
SLOPE = 24
CHARGED = 36
Z_LOW = 40
FIELDS = 48


def kernel(
    atoms_hbm,
    home_hbm,
    other_hbm,
    home_row_hbm,
    picks_hbm,
    fx_hbm,
    fy_hbm,
    inverse_hbm,
    parts_hbm,
    short_ref,
    long_ref,
    home_smem,
    other_smem,
    home_vmem,
    near,
    fields,
    mesh,
    pushes,
    against,
    grads,
    pot_parts,
    send_a,
    recv_a,
    send_b,
    recv_b,
    send_c,
    recv_c,
    send_d,
    recv_d,
    picks,
    forward_x,
    forward_y,
    inverse,
    parts,
    table_sems,
    atom_sem,
    send_sems,
    recv_sems,
    halo_send,
    halo_recv,
):
    grp = lax.axis_index("grp")
    dom = lax.axis_index("dom")
    pen = lax.axis_index("pen")
    z_hi, y_at = pen >> 3, pen & 7
    at_a = z_hi * 16 + dom
    at_b = grp * 8 + y_at

    def peer_a(k):
        t = (at_a + k) & (PEERS - 1)
        return t, {"grp": grp, "dom": t & 15, "pen": (t >> 4) * 8 + y_at}

    def peer_b(k):
        b = (at_b + k) & (PEERS - 1)
        return b, {"grp": b >> 3, "dom": dom, "pen": z_hi * 8 + (b & 7)}

    pen_next = {"grp": grp, "dom": dom, "pen": lax.rem(pen + 1, 16)}
    pen_prev = {"grp": grp, "dom": dom, "pen": lax.rem(pen + 15, 16)}
    dom_next = {"grp": grp, "dom": lax.rem(dom + 1, 16), "pen": pen}
    dom_prev = {"grp": grp, "dom": lax.rem(dom + 15, 16), "pen": pen}

    load_atoms = pltpu.make_async_copy(atoms_hbm, near.at[4], atom_sem)
    load_atoms.start()
    barrier = pltpu.get_barrier_semaphore()

    def greet(k, carry):
        pl.semaphore_signal(barrier, 1, device_id=peer_a(k)[1], device_id_type=MESH)
        pl.semaphore_signal(barrier, 1, device_id=peer_b(k)[1], device_id_type=MESH)
        return carry

    lax.fori_loop(1, PEERS, greet, 0, unroll=True)
    pl.semaphore_signal(barrier, 1, device_id=pen_next, device_id_type=MESH)
    pl.semaphore_signal(barrier, 1, device_id=pen_prev, device_id_type=MESH)

    loads = [
        pltpu.make_async_copy(source, target, table_sems.at[n])
        for n, (source, target) in enumerate(
            (
                (picks_hbm, picks),
                (fx_hbm, forward_x),
                (fy_hbm, forward_y),
                (inverse_hbm, inverse),
                (parts_hbm, parts),
                (home_hbm, home_smem),
                (other_hbm, other_smem),
                (home_row_hbm, home_vmem),
            )
        )
    ]
    for load in loads:
        load.start()
    load_atoms.wait()

    charge = near[4, 3]
    for c, start in ((0, (dom * 8).astype(f32)), (1, (pen * 8).astype(f32)), (2, 3.0)):
        floored, thetas, slopes = spline_terms(near[4, c] * float(NG))
        lowest = floored - start
        for k in range(4):
            place = lowest + float(k)
            theta, slope = thetas[k], slopes[k]
            if c == 1:
                fields[CHARGED + k] = theta * charge
            if c == 2:
                place = jnp.where(place < 0.0, place + float(NG), place)
                high = theta.astype(bf16).astype(f32)
                fields[Z_LOW + k] = theta - high
                theta = high
                high = slope.astype(bf16).astype(f32)
                fields[Z_LOW + 4 + k] = slope - high
                slope = high
            fields[PLACE + 4 * c + k] = place
            fields[THETA + 4 * c + k] = theta
            fields[SLOPE + 4 * c + k] = slope

    z_at = lax.broadcasted_iota(jnp.int32, (NG, TILE), 0).astype(f32).astype(bf16)
    side_at = lax.broadcasted_iota(jnp.int32, (16, TILE), 0).astype(f32)
    corner_at = jnp.minimum(lax.broadcasted_iota(jnp.int32, (16, TILE), 0), 9).astype(f32)
    corner_x = jnp.floor((corner_at + 0.5) * (1.0 / 3.0))
    corner_y = 8.0 + corner_at - 3.0 * corner_x
    corner_x = corner_x + 8.0

    def row(field, tile):
        return fields[field, pl.ds(tile, 1), :]

    def rows_of(field, tile):
        return [row(field + k, tile) for k in range(4)]

    def narrow(field, tile):
        return [r.astype(bf16) for r in rows_of(field, tile)]

    def at_z(tile):
        return [z_at == r for r in narrow(PLACE + 8, tile)]

    def at(axis, where, tile):
        return [where == r for r in rows_of(PLACE + 4 * axis, tile)]

    def across(value, n):
        return jnp.broadcast_to(value[n : n + 1], (8, TILE))

    mesh[...] = jnp.zeros_like(mesh)

    def spread(step, carry):
        z_high, z_low, p_parts = [], [], []
        for n in range(4):
            tile = step * 4 + n
            is_z = at_z(tile)
            z_high.append(one_of(is_z, narrow(THETA + 8, tile)))
            z_low.append(one_of(is_z, narrow(Z_LOW, tile)))
            t_x, t_y = rows_of(THETA, tile), rows_of(CHARGED, tile)
            w_x, w_y = one_of(at(0, side_at, tile), t_x), one_of(at(1, side_at, tile), t_y)
            pieces = [w_x[:8] * across(w_y, y) for y in range(SIDE)]
            pieces += [across(w_x, x) * w_y[:8] for x in range(8, SIDE)]
            pieces += [one_of(at(0, corner_x, tile), t_x) * one_of(at(1, corner_y, tile), t_y)]
            p_parts.append(split(jnp.concatenate(pieces, axis=0)))
        z_high = jnp.concatenate(z_high, axis=1)
        z_low = jnp.concatenate(z_low, axis=1)
        p_high = jnp.concatenate([p[0] for p in p_parts], axis=1)
        p_low = jnp.concatenate([p[1] for p in p_parts], axis=1)
        wide = dot_nt(z_high, jnp.concatenate([p_high, p_low], axis=0))
        mesh[...] += wide[:, :128] + wide[:, 128:] + dot_nt(z_low, p_high)
        return carry

    lax.fori_loop(0, TILES // 4, spread, 0)

    def put(ref, value):
        for n in range(value.shape[0] // 4):
            ref[n] = value[4 * n : 4 * n + 4]

    def taken(ref):
        return jnp.concatenate([ref[n] for n in range(PEERS)], axis=0)

    def exchange(source, target, phase, peer, own, slot):
        def post(k, carry):
            index, device = peer(k)
            pltpu.make_async_remote_copy(
                src_ref=source.at[slot(index)],
                dst_ref=target.at[own],
                send_sem=send_sems.at[phase],
                recv_sem=recv_sems.at[phase],
                device_id=device,
                device_id_type=MESH,
            ).start()
            return carry

        lax.fori_loop(1, PEERS, post, 0)
        target[own] = source[slot(own)]

    def arrived(target, phase, device):
        whole = target.at[pl.ds(0, PEERS - 1)]
        both = pltpu.make_async_remote_copy(
            src_ref=whole,
            dst_ref=whole,
            send_sem=send_sems.at[phase],
            recv_sem=recv_sems.at[phase],
            device_id=device,
            device_id_type=MESH,
        )
        both.wait_recv()
        return both

    def same(index):
        return index

    loads[0].wait()
    put(send_a, to_z(mesh[...], picks[1536:]))
    pl.semaphore_wait(barrier, 2 * (PEERS - 1) + 2)
    exchange(send_a, recv_a, 0, peer_a, at_a, same)

    def halo(source, target, n, device):
        return pltpu.make_async_remote_copy(
            src_ref=near.at[source],
            dst_ref=near.at[target],
            send_sem=halo_send.at[n],
            recv_sem=halo_recv.at[n],
            device_id=device,
            device_id_type=MESH,
        )

    side = [halo(4, 3, 0, pen_next), halo(4, 5, 1, pen_prev)]
    pl.when(y_at != 7)(side[0].start)
    pl.when(y_at != 0)(side[1].start)
    ends = [
        halo(slot, slot - 3 if up else slot + 3, 2 + 2 * n + up, device)
        for n, slot in enumerate((3, 4, 5))
        for up, device in enumerate((dom_prev, dom_next))
    ]

    def hand_on(n):
        if n != 1:
            side[n // 2].wait_recv()
        for copy in ends[2 * n : 2 * n + 2]:
            copy.start()

    table_row = lax.broadcasted_iota(jnp.int32, (16, 4 * TILE), 0)
    table_block = lax.broadcasted_iota(jnp.int32, (16, 4 * TILE), 1) >> 7
    table_sign = jnp.where(table_block == 3, 1.0, -1.0)
    table_fixed = jnp.where(((table_row & 3) == table_block) & (table_row < 12), table_sign, 0.0)

    def home_table(tile, carry):
        rows = [near[4, c, pl.ds(tile, 1), :] for c in range(3)]
        filled = table_fixed
        parts_of = thirds(jnp.concatenate(rows + [jnp.zeros_like(rows[0])], axis=1))
        for k in range(3):
            filled = jnp.where(table_row == 12 + k, parts_of[k], filled)
        against[tile] = filled.astype(bf16)
        return carry

    lax.fori_loop(0, TILES, home_table, 0, unroll=2)

    pl.delay(2400)
    pl.when(y_at == 7)(side[0].start)
    pl.when(y_at == 0)(side[1].start)

    for load in loads[1:]:
        load.wait()
    part_xc, part_xs, part_yc, part_ys = (parts[128 * n : 128 * n + 128, :] for n in range(4))
    lane = lax.broadcasted_iota(jnp.int32, (1, NG), 1)
    k_x = at_b * 4 + (lane // 4)
    k_z = at_a * 4 + lax.rem(lane, 4)
    k_y = lax.broadcasted_iota(jnp.int32, (NG, 1), 0)
    used = lane < 16
    factor = green_of(jnp.where(used, k_x, 1), k_y, jnp.where(used, k_z, 1))

    peer_one_a = peer_a(1)[1]
    peer_one_b = peer_b(1)[1]
    sent_0 = arrived(recv_a, 0, peer_one_a)
    put(send_b, to_lines_x(taken(recv_a), forward_x[...], part_xc, part_xs, picks[:1024]))
    exchange(send_b, recv_b, 1, peer_b, at_b, same)
    hand_on(1)
    pl.when(y_at != 0)(lambda: hand_on(0))
    pl.when(y_at != 7)(lambda: hand_on(2))

    sent_1 = arrived(recv_b, 1, peer_one_b)
    put(
        send_c,
        through_y(
            taken(recv_b),
            factor,
            forward_y[...],
            inverse[128:],
            part_yc,
            part_ys,
            picks[1024:1536],
        ),
    )
    exchange(send_c, recv_c, 2, peer_b, at_b, lambda index: index & 7)

    pl.when(y_at == 0)(lambda: hand_on(0))
    pl.when(y_at == 7)(lambda: hand_on(2))

    sent_2 = arrived(recv_c, 2, peer_one_b)
    put(send_d, from_lines_x(taken(recv_c), inverse[:128], part_xc, part_xs, picks[:1024]))
    exchange(send_d, recv_d, 3, peer_a, at_a, same)

    for copy in ends:
        copy.wait()
    for copy in side:
        copy.wait_send()
    def period(step, at_edge):
        below = (step == -1) & (at_edge == 0)
        above = (step == 1) & (at_edge == 15)
        return jnp.where(below, 1.0, jnp.where(above, -1.0, 0.0)).astype(f32)

    def pair(n, carry):
        home, other = home_smem[n], other_smem[n]
        block, tile = other >> 5, other & 31
        step_d = jnp.where(block < 3, -1, jnp.where(block < 6, 0, 1))
        step_p = block - 3 * (step_d + 1) - 1
        far = [near[block, c, pl.ds(tile, 1), :] for c in range(4)]
        far[0] = far[0] - period(step_d, dom)
        far[1] = far[1] - period(step_p, pen)
        rows = pair_push(jnp.concatenate(far, axis=0), against[home])
        for c in range(3):
            pushes[c, pl.ds(n, 1), :] = rows[c]
        return carry

    lax.fori_loop(0, PAIRS, pair, 0, unroll=4)
    tile_ids = lax.broadcasted_iota(jnp.int32, (TILES, PAIRS), 0)
    owners = jnp.where(home_vmem[...] == tile_ids, 1.0, 0.0).astype(bf16)
    for c in range(3):
        high, low = split(pushes[c])
        short_ref[c] = (dot(owners, high) + dot(owners, low)) * (charge * (32.0 * 2.0 / math.sqrt(256.0)))

    sent_3 = arrived(recv_d, 3, peer_one_a)
    pot_high, pot_low = split(from_z(taken(recv_d), picks[1536:]))
    pot_parts[:128] = pot_high
    pot_parts[128:] = pot_low

    def interpolate(step, carry):
        for n in range(2):
            tile = step * 2 + n
            is_z = at_z(tile)
            high = [one_of(is_z, narrow(THETA + 8, tile)), one_of(is_z, narrow(SLOPE + 8, tile))]
            low = [one_of(is_z, narrow(Z_LOW, tile)), one_of(is_z, narrow(Z_LOW + 4, tile))]
            full = dot(pot_parts[...], jnp.concatenate(high, axis=1))
            along = full[:128] + full[128:] + dot(pot_parts[:128], jnp.concatenate(low, axis=1))
            value = [along[8 * k : 8 * k + 8, :128] for k in range(16)]
            slope = [along[8 * k : 8 * k + 8, 128:] for k in range(16)]
            t_x, d_x = rows_of(THETA, tile), rows_of(SLOPE, tile)
            t_y, d_y = rows_of(THETA + 4, tile), rows_of(SLOPE + 4, tile)
            is_x, is_y = at(0, side_at, tile), at(1, side_at, tile)
            w_x, s_x = one_of(is_x, t_x), one_of(is_x, d_x)
            w_y, s_y = one_of(is_y, t_y), one_of(is_y, d_y)
            by_y = [[], [], []]
            for y in range(SIDE):
                by_y[0].append(across(w_y, y) * value[y])
                by_y[1].append(across(s_y, y) * value[y])
                by_y[2].append(across(w_y, y) * slope[y])
            by_x = [[], [], []]
            for x in range(8, SIDE):
                by_x[0].append(across(s_x, x) * value[x + 3])
                by_x[1].append(across(w_x, x) * value[x + 3])
                by_x[2].append(across(w_x, x) * slope[x + 3])
            is_x, is_y = at(0, corner_x, tile), at(1, corner_y, tile)
            cw_x, cs_x = one_of(is_x, t_x), one_of(is_x, d_x)
            cw_y, cs_y = one_of(is_y, t_y), one_of(is_y, d_y)
            ends_x, ends_y = (s_x, w_x, w_x), (w_y, s_y, w_y)
            for c in range(3):
                total = ends_x[c][:8] * sum(by_y[c][1:], by_y[c][0])
                total += ends_y[c][:8] * sum(by_x[c][1:], by_x[c][0])
                own = slope if c == 2 else value
                corner = (cs_x * cw_y, cw_x * cs_y, cw_x * cw_y)[c]
                total += corner[:8] * own[14] + corner[8:] * own[15]
                grads[c, pl.ds(tile, 1), :] = jnp.sum(total, axis=0, keepdims=True)
        return carry

    lax.fori_loop(0, TILES // 2, interpolate, 0)
    for sent in (sent_0, sent_1, sent_2, sent_3):
        sent.wait_send()
    total_atoms = 4 * 16 * 16 * 4096
    scale = -0.4 * NG / math.sqrt(NG * total_atoms)
    for c in range(3):
        long_ref[c] = grads[c] * (charge * scale)


def on_device(atoms, pair_home, pair_other, *tables):
    hbm = pl.BlockSpec(memory_space=pl.ANY)
    vmem = pl.BlockSpec(memory_space=pltpu.VMEM)
    blocks = atoms.reshape(4, TILES, TILE)
    homes = pair_home.reshape(PAIRS)
    others = pair_other.reshape(PAIRS)
    force = jax.ShapeDtypeStruct((3, TILES, TILE), f32)
    message = pltpu.VMEM((PEERS, 4, NG), f32)
    short, long = pl.pallas_call(
        kernel,
        out_shape=(force, force),
        in_specs=[hbm] * (4 + len(NAMES)),
        out_specs=(vmem, vmem),
        scratch_shapes=[
            pltpu.SMEM((PAIRS,), jnp.int32),
            pltpu.SMEM((PAIRS,), jnp.int32),
            pltpu.VMEM((1, PAIRS), jnp.int32),
            pltpu.VMEM((9, 4, TILES, TILE), f32),
            pltpu.VMEM((FIELDS, TILES, TILE), f32),
            pltpu.VMEM((NG, NG), f32),
            pltpu.VMEM((3, PAIRS, TILE), f32),
            pltpu.VMEM((TILES, 16, 4 * TILE), bf16),
            pltpu.VMEM((3, TILES, TILE), f32),
            pltpu.VMEM((2 * NG, NG), bf16),
            message,
            message,
            message,
            message,
            pltpu.VMEM((8, 4, NG), f32),
            message,
            message,
            message,
            *[pltpu.VMEM(t.shape, t.dtype) for t in tables],
            pltpu.SemaphoreType.DMA((len(NAMES) + 3,)),
            pltpu.SemaphoreType.DMA,
            pltpu.SemaphoreType.DMA((4,)),
            pltpu.SemaphoreType.DMA((4,)),
            pltpu.SemaphoreType.DMA((8,)),
            pltpu.SemaphoreType.DMA((8,)),
        ],
        compiler_params=pltpu.CompilerParams(
            collective_id=0, has_side_effects=True, vmem_limit_bytes=56_400_000
        ),
        name="forces",
    )(blocks, homes, others, homes.reshape(1, PAIRS), *tables)
    return short.reshape(3, 1, 1, TILES * TILE), long.reshape(3, 1, 1, TILES * TILE)


def solution(mesh):
    tables = make_tables()

    def whole(atoms, pair_home, pair_other):
        fixed = [jnp.asarray(tables[name]) for name in NAMES]
        mapped = jax.shard_map(
            lambda a, h, o: on_device(a, h, o, *fixed),
            mesh=mesh,
            in_specs=(P(None, "grp", "dom", "pen"), P("grp", "dom", "pen"), P("grp", "dom", "pen")),
            out_specs=(P(None, "grp", "dom", "pen"), P(None, "grp", "dom", "pen")),
            check_vma=False,
        )
        return mapped(atoms, pair_home, pair_other)

    return whole
```

```python
import functools
import math

import jax
import jax.numpy as jnp
import numpy as np
from jax import lax
from jax.experimental import pallas as pl
from jax.experimental.pallas import tpu as pltpu
from jax.sharding import PartitionSpec as P

NG = 128
TILE = 128
TILES = 32
PAIRS = 64
SIDE = 11
PEERS = 32
MESH = pl.DeviceIdType.MESH
f32 = jnp.float32
bf16 = jnp.bfloat16


def basis(cells):
    k = np.arange(NG)[:, None]
    m = np.where(k <= NG // 2, k, k - NG // 2)
    angle = 2.0 * np.pi * np.mod(m * cells[None, :], NG) / NG
    return np.where(k <= NG // 2, np.cos(angle), np.sin(angle))


def turning(starts, lanes, used):
    k = np.arange(NG)[:, None]
    m = np.where(k <= NG // 2, k, k - NG // 2)
    first = 2.0 * np.pi * np.mod(m * starts[None, :], NG) / NG
    second = 2.0 * np.pi * np.mod(m * lanes[None, :], NG) / NG
    is_cos = k <= NG // 2
    part_c = np.where(is_cos, np.cos(second), np.sin(second)) * used[None, :]
    part_s = np.where(is_cos, -np.sin(second), np.cos(second)) * used[None, :]
    return np.cos(first), np.sin(first), part_c, part_s


def halves(table):
    table = np.asarray(table, np.float32)
    high = table.astype(jnp.bfloat16)
    low = (table - high.astype(np.float32)).astype(jnp.bfloat16)
    return high, low


def spread_columns(turn_c, turn_s, inner):
    count = turn_c.shape[1]
    out = np.zeros((inner, 2, NG, count, inner))
    for i in range(inner):
        out[i, 0, :, :, i] = turn_c
        out[i, 1, :, :, i] = turn_s
    return out.reshape(inner * 2 * NG, count * inner)


def patch_places():
    places = [(x, y) for y in range(SIDE) for x in range(8)]
    places += [(x, y) for x in range(8, SIDE) for y in range(8)]
    places += [(x, y) for x in range(8, SIDE) for y in range(8, SIDE)]
    places += [(SIDE, SIDE)] * (NG - len(places))
    return np.array(places).T


def make_tables():
    row = np.arange(NG)
    row_x, row_y = patch_places()
    lane_z, lane_y = (row // 16) % 2, row % 16
    x_c, x_s, bx_c, bx_s = turning(8 * np.arange(16), row_x - 3, row < SIDE * SIDE)
    y_c, y_s, by_c, by_s = turning(8 * np.arange(8), 64 * lane_z - 3 + lane_y, lane_y < SIDE)
    x_cols, y_cols = spread_columns(x_c, x_s, 4), spread_columns(y_c, y_s, 4)
    xh, xl = halves(x_cols)
    yh, yl = halves(y_cols)
    forward_x = np.concatenate([xh, xh, xl], axis=1)
    forward_y = np.concatenate([yh, yh, yl], axis=1)
    inverse_x = np.concatenate([xh.T, xl.T], axis=0)
    inverse_y = np.concatenate([yh.T, yl.T], axis=0)
    pick_x = np.zeros((4, 2, NG, NG), np.float32)
    for j in range(4):
        for z in range(2):
            for r in range(SIDE * SIDE):
                pick_x[j, z, r, j * 32 + z * 16 + row_y[r]] = 1.0
    pick_y = np.zeros((4, NG, NG), np.float32)
    for i in range(4):
        for lane in range(NG):
            pick_y[i, lane, i * 4 + lane // 32] = 1.0
    zh, zl = halves(basis(row))
    return dict(
        forward_x=forward_x,
        forward_y=forward_y,
        inverse=np.concatenate([inverse_x, inverse_y], axis=0),
        picks=np.concatenate(
            [
                pick_x.reshape(1024, NG).astype(jnp.bfloat16),
                pick_y.reshape(512, NG).astype(jnp.bfloat16),
                zh,
                zl,
            ],
            axis=0,
        ),
        parts=np.concatenate([bx_c, bx_s, by_c, by_s], axis=0).astype(np.float32),
    )


NAMES = (
    "picks",
    "forward_x",
    "forward_y",
    "inverse",
    "parts",
)


def dot(a, b):
    return lax.dot_general(a, b, (((1,), (0,)), ((), ())), preferred_element_type=f32)


def dot_nt(a, b):
    return lax.dot_general(a, b, (((1,), (1,)), ((), ())), preferred_element_type=f32)


def split(x):
    high = x.astype(bf16)
    return high, (x - high.astype(f32)).astype(bf16)


def stacked(x):
    high = x.astype(bf16).astype(f32)
    return jnp.concatenate([high, x - high, high], axis=0).astype(bf16)


def spline_terms(scaled):
    floored = jnp.floor(scaled)
    w = scaled - floored
    remain = 1.0 - w
    sq = w * w
    cube = sq * w
    thetas = [
        remain * remain * remain * (1.0 / 6.0),
        (3.0 * cube - 6.0 * sq + 4.0) * (1.0 / 6.0),
        (-3.0 * cube + 3.0 * sq + 3.0 * w + 1.0) * (1.0 / 6.0),
        cube * (1.0 / 6.0),
    ]
    slopes = [
        -0.5 * remain * remain,
        1.5 * sq - 2.0 * w,
        -1.5 * sq + w + 0.5,
        0.5 * sq,
    ]
    return floored, thetas, slopes


def one_of(is_at, values):
    out = jnp.where(is_at[3], values[3], 0.0)
    for k in (2, 1, 0):
        out = jnp.where(is_at[k], values[k], out)
    return out


def matches(t):
    return [t == k for k in range(4)]


def to_lines_x(got, forward_x, part_c, part_s, pick_x):
    both = jnp.concatenate([got[:64], got[64:]], axis=1)
    turned = dot(forward_x, stacked(both))
    c2, s2 = jnp.concatenate([part_c] * 2, axis=1), jnp.concatenate([part_s] * 2, axis=1)
    out = None
    for j in range(4):
        q = c2 * turned[j * 256 : j * 256 + 128] + s2 * turned[j * 256 + 128 : j * 256 + 256]
        high, low = split(q)
        pick = pick_x[j * 256 : (j + 1) * 256]
        term = dot(high, pick) + dot(low, pick)
        out = term if out is None else out + term
    return out


def through_y(got, factor, forward_y, inverse_y, part_c, part_s, pick_y):
    total = (got[:32] + got[32:64]) + (got[64:96] + got[96:])
    turned = dot(forward_y, stacked(total))
    lines = jnp.concatenate(
        [
            part_c * turned[i * 256 : i * 256 + 128] + part_s * turned[i * 256 + 128 : i * 256 + 256]
            for i in range(4)
        ],
        axis=1,
    )
    high, low = split(lines)
    freq = (dot(high, pick_y) + dot(low, pick_y)) * factor
    high, low = split(freq)
    wide = dot_nt(high, pick_y) + dot_nt(low, pick_y)
    out = None
    for i in range(4):
        piece = wide[:, i * 128 : (i + 1) * 128]
        high, low = split(jnp.concatenate([part_c * piece, part_s * piece], axis=0))
        table = inverse_y[:, i * 256 : (i + 1) * 256]
        full = dot(table, high)
        term = full[:32] + full[32:] + dot(table[:32], low)
        out = term if out is None else out + term
    return out


def from_lines_x(got, inverse_x, part_c, part_s, pick_x):
    high, low = split(got)
    c2, s2 = jnp.concatenate([part_c] * 2, axis=1), jnp.concatenate([part_s] * 2, axis=1)
    out = None
    for j in range(4):
        pick = pick_x[j * 256 : (j + 1) * 256]
        wide = dot_nt(high, pick) + dot_nt(low, pick)
        q_high, q_low = split(jnp.concatenate([c2 * wide, s2 * wide], axis=0))
        table = inverse_x[:, j * 256 : (j + 1) * 256]
        full = dot(table, q_high)
        term = full[:64] + full[64:] + dot(table[:64], q_low)
        out = term if out is None else out + term
    return jnp.concatenate([out[:, :128], out[:, 128:]], axis=0)


def to_z(mesh, basis_z):
    high, low = split(mesh)
    full = dot(basis_z, high)
    return full[:128] + full[128:] + dot(basis_z[:128], low)


def from_z(got, basis_z):
    high, low = split(got.T)
    return dot(high, basis_z[:128]) + dot(high, basis_z[128:]) + dot(low, basis_z[:128])


def green_of(k_x, k_y, k_z):
    def mode(k):
        return jnp.where(k <= NG // 2, k, k - NG // 2)

    def weight(m):
        ratio = (2.0 + jnp.cos(m.astype(f32) * (2.0 * math.pi / NG))) / 3.0
        twice = jnp.where((m == 0) | (m == NG // 2), 1.0, 2.0)
        return twice / (ratio * ratio)

    m_x, m_y, m_z = mode(k_x), mode(k_y), mode(k_z)
    square = (m_x * m_x + m_z * m_z + m_y * m_y).astype(f32)
    beta = 0.6 * NG
    value = jnp.exp(square * (-math.pi * math.pi / (beta * beta)))
    value = value / (math.pi * jnp.maximum(square, 1.0))
    value = value * (weight(m_x) * weight(m_z)) * weight(m_y)
    return jnp.where(square > 0.5, value, 0.0)


def thirds(x):
    high = x.astype(bf16).astype(f32)
    rest = x - high
    middle = rest.astype(bf16).astype(f32)
    return high, middle, rest - middle


def pair_push(other, against):
    columns = jnp.concatenate([*thirds(other), jnp.ones_like(other)], axis=0).astype(bf16)
    wide = lax.dot_general(
        columns, against, (((0,), (0,)), ((), ())), preferred_element_type=f32
    )
    delta = [wide[:, 128 * c : 128 * c + 128] for c in range(3)]
    delta[2] = delta[2] - jnp.floor(delta[2] + 0.5)
    square = delta[0] * delta[0] + delta[1] * delta[1] + delta[2] * delta[2]
    weight = jnp.exp2(square * (-512.0 * math.log2(math.e))) * wide[:, 384:]
    return [jnp.sum(d * weight, axis=0, keepdims=True) for d in delta]


PLACE = 0
THETA = 12
SLOPE = 24
CHARGED = 36
Z_LOW = 40
FIELDS = 48


def kernel(
    atoms_hbm,
    home_hbm,
    other_hbm,
    home_row_hbm,
    picks_hbm,
    fx_hbm,
    fy_hbm,
    inverse_hbm,
    parts_hbm,
    short_ref,
    long_ref,
    home_smem,
    other_smem,
    home_vmem,
    near,
    fields,
    mesh,
    pushes,
    against,
    grads,
    pot_parts,
    z_table,
    xy_table,
    send_a,
    recv_a,
    send_b,
    recv_b,
    send_c,
    recv_c,
    send_d,
    recv_d,
    picks,
    forward_x,
    forward_y,
    inverse,
    parts,
    table_sems,
    atom_sem,
    send_sems,
    recv_sems,
    halo_send,
    halo_recv,
):
    grp = lax.axis_index("grp")
    dom = lax.axis_index("dom")
    pen = lax.axis_index("pen")
    z_hi, y_at = pen >> 3, pen & 7
    at_a = z_hi * 16 + dom
    at_b = grp * 8 + y_at

    def peer_a(k):
        t = (at_a + k) & (PEERS - 1)
        return t, {"grp": grp, "dom": t & 15, "pen": (t >> 4) * 8 + y_at}

    def peer_b(k):
        to_grp, to_y = (grp + (k >> 3)) & 3, (y_at + (k & 7)) & 7
        return to_grp * 8 + to_y, {"grp": to_grp, "dom": dom, "pen": z_hi * 8 + to_y}

    pen_next = {"grp": grp, "dom": dom, "pen": lax.rem(pen + 1, 16)}
    pen_prev = {"grp": grp, "dom": dom, "pen": lax.rem(pen + 15, 16)}
    dom_next = {"grp": grp, "dom": lax.rem(dom + 1, 16), "pen": pen}
    dom_prev = {"grp": grp, "dom": lax.rem(dom + 15, 16), "pen": pen}

    load_atoms = pltpu.make_async_copy(atoms_hbm, near.at[4], atom_sem)
    load_atoms.start()
    barrier = pltpu.get_barrier_semaphore()

    for n in range(1, PEERS):
        k = 16 + (n >> 1) * (1 if n & 1 else -1)
        pl.semaphore_signal(barrier, 1, device_id=peer_a(k)[1], device_id_type=MESH)
    for k in range(1, PEERS):
        pl.semaphore_signal(barrier, 1, device_id=peer_b(k)[1], device_id_type=MESH)
    pl.semaphore_signal(barrier, 1, device_id=pen_next, device_id_type=MESH)
    pl.semaphore_signal(barrier, 1, device_id=pen_prev, device_id_type=MESH)

    loads = [
        pltpu.make_async_copy(source, target, table_sems.at[n])
        for n, (source, target) in enumerate(
            (
                (picks_hbm, picks),
                (fx_hbm, forward_x),
                (fy_hbm, forward_y),
                (inverse_hbm, inverse),
                (parts_hbm, parts),
                (home_hbm, home_smem),
                (other_hbm, other_smem),
                (home_row_hbm, home_vmem),
            )
        )
    ]
    for load in loads:
        load.start()
    load_atoms.wait()

    charge = near[4, 3]
    for c, start in ((0, (dom * 8).astype(f32)), (1, (pen * 8).astype(f32)), (2, 3.0)):
        floored, thetas, slopes = spline_terms(near[4, c] * float(NG))
        lowest = floored - start
        for k in range(4):
            place = lowest + float(k)
            theta, slope = thetas[k], slopes[k]
            if c == 1:
                fields[CHARGED + k] = theta * charge
            if c == 2:
                place = jnp.where(place < 0.0, place + float(NG), place)
                high = theta.astype(bf16).astype(f32)
                fields[Z_LOW + k] = theta - high
                theta = high
                high = slope.astype(bf16).astype(f32)
                fields[Z_LOW + 4 + k] = slope - high
                slope = high
            fields[PLACE + 4 * c + k] = place
            fields[THETA + 4 * c + k] = theta
            fields[SLOPE + 4 * c + k] = slope

    z_at = lax.broadcasted_iota(jnp.int32, (NG, TILE), 0).astype(f32).astype(bf16)
    side_at = lax.broadcasted_iota(jnp.int32, (16, TILE), 0).astype(f32)
    corner_at = jnp.minimum(lax.broadcasted_iota(jnp.int32, (16, TILE), 0), 9).astype(f32)
    corner_x = jnp.floor((corner_at + 0.5) * (1.0 / 3.0))
    corner_y = 8.0 + corner_at - 3.0 * corner_x
    corner_x = corner_x + 8.0

    def row(field, tile):
        return fields[field, pl.ds(tile, 1), :]

    def rows_of(field, tile):
        return [row(field + k, tile) for k in range(4)]

    def narrow(field, tile):
        return [r.astype(bf16) for r in rows_of(field, tile)]

    def at_z(tile):
        return [z_at == r for r in narrow(PLACE + 8, tile)]

    def at(axis, where, tile):
        return [where == r for r in rows_of(PLACE + 4 * axis, tile)]

    def across(value, n):
        return jnp.broadcast_to(value[n : n + 1], (8, TILE))

    mesh[...] = jnp.zeros_like(mesh)

    def spread(step, carry):
        z_high, z_low, p_parts = [], [], []
        for n in range(4):
            tile = step * 4 + n
            is_z = at_z(tile)
            z_high.append(one_of(is_z, narrow(THETA + 8, tile)))
            z_low.append(one_of(is_z, narrow(Z_LOW, tile)))
            z_table[tile, :128, :128] = z_high[-1]
            z_table[tile, 128:, :128] = z_low[-1]
            t_x, t_y = rows_of(THETA, tile), rows_of(CHARGED, tile)
            w_x, w_y = one_of(at(0, side_at, tile), t_x), one_of(at(1, side_at, tile), t_y)
            pieces = [w_x[:8] * across(w_y, y) for y in range(SIDE)]
            pieces += [across(w_x, x) * w_y[:8] for x in range(8, SIDE)]
            pieces += [one_of(at(0, corner_x, tile), t_x) * one_of(at(1, corner_y, tile), t_y)]
            p_parts.append(split(jnp.concatenate(pieces, axis=0)))
        z_high = jnp.concatenate(z_high, axis=1)
        z_low = jnp.concatenate(z_low, axis=1)
        p_high = jnp.concatenate([p[0] for p in p_parts], axis=1)
        p_low = jnp.concatenate([p[1] for p in p_parts], axis=1)
        wide = dot_nt(z_high, jnp.concatenate([p_high, p_low], axis=0))
        mesh[...] += wide[:, :128] + wide[:, 128:] + dot_nt(z_low, p_high)
        return carry

    lax.fori_loop(0, TILES // 4, spread, 0)

    def put(ref, value):
        for n in range(value.shape[0] // 4):
            ref[n] = value[4 * n : 4 * n + 4]

    def taken(ref):
        return jnp.concatenate([ref[n] for n in range(PEERS)], axis=0)

    def exchange(source, target, phase, peer, own, slot, offset):
        def post(k, carry):
            index, device = peer(offset(k))
            pltpu.make_async_remote_copy(
                src_ref=source.at[slot(index)],
                dst_ref=target.at[own],
                send_sem=send_sems.at[phase],
                recv_sem=recv_sems.at[phase],
                device_id=device,
                device_id_type=MESH,
            ).start()
            return carry

        lax.fori_loop(0, PEERS - 1, post, 0)
        target[own] = source[slot(own)]

    def arrived(target, phase, device):
        whole = target.at[pl.ds(0, PEERS - 1)]
        both = pltpu.make_async_remote_copy(
            src_ref=whole,
            dst_ref=whole,
            send_sem=send_sems.at[phase],
            recv_sem=recv_sems.at[phase],
            device_id=device,
            device_id_type=MESH,
        )
        both.wait_recv()
        return both

    def same(index):
        return index

    def outward(n, middle):
        return middle + ((n + 1) >> 1) * (1 - 2 * (n & 1))

    def far_first(k):
        return outward(k, 16)

    def far_plane(k):
        return (outward(k & 3, 2) & 3) * 8 + (outward(k >> 2, 4) & 7)

    def low_first(k):
        return PEERS + k + (k >= at_a).astype(jnp.int32) - at_a

    loads[0].wait()
    put(send_a, to_z(mesh[...], picks[1536:]))
    pl.semaphore_wait(barrier, 2 * (PEERS - 1) + 2)
    exchange(send_a, recv_a, 0, peer_a, at_a, same, far_first)

    def halo(source, target, n, device):
        return pltpu.make_async_remote_copy(
            src_ref=near.at[source],
            dst_ref=near.at[target],
            send_sem=halo_send.at[n],
            recv_sem=halo_recv.at[n],
            device_id=device,
            device_id_type=MESH,
        )

    side = [halo(4, 3, 0, pen_next), halo(4, 5, 1, pen_prev)]
    pl.when(y_at != 7)(side[0].start)
    pl.when(y_at != 0)(side[1].start)
    ends = [
        halo(slot, slot - 3 if up else slot + 3, 2 + 2 * n + up, device)
        for n, slot in enumerate((3, 4, 5))
        for up, device in enumerate((dom_prev, dom_next))
    ]

    def hand_on(n):
        if n != 1:
            side[n // 2].wait_recv()
        for copy in ends[2 * n : 2 * n + 2]:
            copy.start()

    table_row = lax.broadcasted_iota(jnp.int32, (16, 4 * TILE), 0)
    table_block = lax.broadcasted_iota(jnp.int32, (16, 4 * TILE), 1) >> 7
    table_sign = jnp.where(table_block == 3, 1.0, -1.0)
    table_fixed = jnp.where(((table_row & 3) == table_block) & (table_row < 12), table_sign, 0.0)

    def home_table(tile, carry):
        rows = [near[4, c, pl.ds(tile, 1), :] for c in range(3)]
        filled = table_fixed
        parts_of = thirds(jnp.concatenate(rows + [jnp.zeros_like(rows[0])], axis=1))
        for k in range(3):
            filled = jnp.where(table_row == 12 + k, parts_of[k], filled)
        against[tile] = filled.astype(bf16)
        return carry

    lax.fori_loop(0, TILES, home_table, 0, unroll=2)

    def prepare(step, carry):
        for n in range(2):
            tile = step * 2 + n
            is_z = at_z(tile)
            z_table[tile, :128, 128:] = one_of(is_z, narrow(SLOPE + 8, tile))
            z_table[tile, 128:, 128:] = one_of(is_z, narrow(Z_LOW + 4, tile))
            t_x, d_x = rows_of(THETA, tile), rows_of(SLOPE, tile)
            t_y, d_y = rows_of(THETA + 4, tile), rows_of(SLOPE + 4, tile)
            is_x, is_y = at(0, side_at, tile), at(1, side_at, tile)
            xy_table[tile, 0:16] = one_of(is_x, t_x)
            xy_table[tile, 16:32] = one_of(is_x, d_x)
            xy_table[tile, 32:48] = one_of(is_y, t_y)
            xy_table[tile, 48:64] = one_of(is_y, d_y)
            is_x, is_y = at(0, corner_x, tile), at(1, corner_y, tile)
            cw_x, cs_x = one_of(is_x, t_x), one_of(is_x, d_x)
            cw_y, cs_y = one_of(is_y, t_y), one_of(is_y, d_y)
            xy_table[tile, 64:80] = cs_x * cw_y
            xy_table[tile, 80:96] = cw_x * cs_y
            xy_table[tile, 96:112] = cw_x * cw_y
        return carry

    lax.fori_loop(0, TILES // 2, prepare, 0)

    pl.delay(1000)
    pl.when(y_at == 7)(side[0].start)
    pl.when(y_at == 0)(side[1].start)

    for load in loads[1:]:
        load.wait()
    part_xc, part_xs, part_yc, part_ys = (parts[128 * n : 128 * n + 128, :] for n in range(4))
    lane = lax.broadcasted_iota(jnp.int32, (1, NG), 1)
    k_x = at_b * 4 + (lane // 4)
    k_z = at_a * 4 + lax.rem(lane, 4)
    k_y = lax.broadcasted_iota(jnp.int32, (NG, 1), 0)
    used = lane < 16
    factor = green_of(jnp.where(used, k_x, 1), k_y, jnp.where(used, k_z, 1))

    peer_one_a = peer_a(1)[1]
    peer_one_b = peer_b(1)[1]
    sent_0 = arrived(recv_a, 0, peer_one_a)
    put(send_b, to_lines_x(taken(recv_a), forward_x[...], part_xc, part_xs, picks[:1024]))
    exchange(send_b, recv_b, 1, peer_b, at_b, same, far_plane)
    hand_on(1)
    pl.when(y_at != 0)(lambda: hand_on(0))
    pl.when(y_at != 7)(lambda: hand_on(2))

    sent_1 = arrived(recv_b, 1, peer_one_b)
    put(
        send_c,
        through_y(
            taken(recv_b),
            factor,
            forward_y[...],
            inverse[128:],
            part_yc,
            part_ys,
            picks[1024:1536],
        ),
    )
    exchange(send_c, recv_c, 2, peer_b, at_b, lambda index: index & 7, far_plane)

    pl.when(y_at == 0)(lambda: hand_on(0))
    pl.when(y_at == 7)(lambda: hand_on(2))

    sent_2 = arrived(recv_c, 2, peer_one_b)
    put(send_d, from_lines_x(taken(recv_c), inverse[:128], part_xc, part_xs, picks[:1024]))
    exchange(send_d, recv_d, 3, peer_a, at_a, same, low_first)

    for copy in ends:
        copy.wait()
    for copy in side:
        copy.wait_send()
    def period(step, at_edge):
        below = (step == -1) & (at_edge == 0)
        above = (step == 1) & (at_edge == 15)
        return jnp.where(below, 1.0, jnp.where(above, -1.0, 0.0)).astype(f32)

    def pair(n, carry):
        home, other = home_smem[n], other_smem[n]
        block, tile = other >> 5, other & 31
        step_d = jnp.where(block < 3, -1, jnp.where(block < 6, 0, 1))
        step_p = block - 3 * (step_d + 1) - 1
        far = [near[block, c, pl.ds(tile, 1), :] for c in range(4)]
        far[0] = far[0] - period(step_d, dom)
        far[1] = far[1] - period(step_p, pen)
        rows = pair_push(jnp.concatenate(far, axis=0), against[home])
        for c in range(3):
            pushes[c, pl.ds(n, 1), :] = rows[c]
        return carry

    lax.fori_loop(0, PAIRS, pair, 0, unroll=4)
    tile_ids = lax.broadcasted_iota(jnp.int32, (TILES, PAIRS), 0)
    owners = jnp.where(home_vmem[...] == tile_ids, 1.0, 0.0).astype(bf16)
    for c in range(3):
        high, low = split(pushes[c])
        short_ref[c] = (dot(owners, high) + dot(owners, low)) * charge

    sent_3 = arrived(recv_d, 3, peer_one_a)
    pot_high, pot_low = split(from_z(taken(recv_d), picks[1536:]))
    pot_parts[:, :128] = pot_high
    pot_parts[:, 128:] = pot_low

    def interpolate(step, carry):
        for n in range(2):
            tile = step * 2 + n
            high, low = z_table[tile, :128], z_table[tile, 128:]
            along = dot(pot_parts[...], jnp.concatenate([high, high], axis=0))
            along += dot(pot_parts[:, :128], low)
            value = [along[8 * k : 8 * k + 8, :128] for k in range(16)]
            slope = [along[8 * k : 8 * k + 8, 128:] for k in range(16)]
            w_x, s_x, w_y, s_y = (xy_table[tile, 16 * k : 16 * k + 16] for k in range(4))
            by_y = [[], [], []]
            for y in range(SIDE):
                by_y[0].append(across(w_y, y) * value[y])
                by_y[1].append(across(s_y, y) * value[y])
                by_y[2].append(across(w_y, y) * slope[y])
            by_x = [[], [], []]
            for x in range(8, SIDE):
                by_x[0].append(across(s_x, x) * value[x + 3])
                by_x[1].append(across(w_x, x) * value[x + 3])
                by_x[2].append(across(w_x, x) * slope[x + 3])
            ends_x, ends_y = (s_x, w_x, w_x), (w_y, s_y, w_y)
            for c in range(3):
                total = ends_x[c][:8] * sum(by_y[c][1:], by_y[c][0])
                total += ends_y[c][:8] * sum(by_x[c][1:], by_x[c][0])
                own = slope if c == 2 else value
                corner = xy_table[tile, 64 + 16 * c : 80 + 16 * c]
                total += corner[:8] * own[14] + corner[8:] * own[15]
                grads[c, pl.ds(tile, 1), :] = jnp.sum(total, axis=0, keepdims=True)
        return carry

    lax.fori_loop(0, TILES // 2, interpolate, 0)
    for sent in (sent_0, sent_1, sent_2, sent_3):
        sent.wait_send()
    for c in range(3):
        long_ref[c] = grads[c] * charge


def on_device(atoms, pair_home, pair_other, *tables):
    hbm = pl.BlockSpec(memory_space=pl.ANY)
    vmem = pl.BlockSpec(memory_space=pltpu.VMEM)
    blocks = atoms.reshape(4, TILES, TILE)
    homes = pair_home.reshape(PAIRS)
    others = pair_other.reshape(PAIRS)
    force = jax.ShapeDtypeStruct((3, TILES, TILE), f32)
    message = pltpu.VMEM((PEERS, 4, NG), f32)
    short, long = pl.pallas_call(
        kernel,
        out_shape=(force, force),
        in_specs=[hbm] * (4 + len(NAMES)),
        out_specs=(vmem, vmem),
        scratch_shapes=[
            pltpu.SMEM((PAIRS,), jnp.int32),
            pltpu.SMEM((PAIRS,), jnp.int32),
            pltpu.VMEM((1, PAIRS), jnp.int32),
            pltpu.VMEM((9, 4, TILES, TILE), f32),
            pltpu.VMEM((FIELDS, TILES, TILE), f32),
            pltpu.VMEM((NG, NG), f32),
            pltpu.VMEM((3, PAIRS, TILE), f32),
            pltpu.VMEM((TILES, 16, 4 * TILE), bf16),
            pltpu.VMEM((3, TILES, TILE), f32),
            pltpu.VMEM((NG, 2 * NG), bf16),
            pltpu.VMEM((TILES, 2 * NG, 2 * TILE), bf16),
            pltpu.VMEM((TILES, 112, TILE), f32),
            message,
            message,
            message,
            message,
            pltpu.VMEM((8, 4, NG), f32),
            message,
            message,
            message,
            *[pltpu.VMEM(t.shape, t.dtype) for t in tables],
            pltpu.SemaphoreType.DMA((len(NAMES) + 3,)),
            pltpu.SemaphoreType.DMA,
            pltpu.SemaphoreType.DMA((4,)),
            pltpu.SemaphoreType.DMA((4,)),
            pltpu.SemaphoreType.DMA((8,)),
            pltpu.SemaphoreType.DMA((8,)),
        ],
        compiler_params=pltpu.CompilerParams(
            collective_id=0, has_side_effects=True, vmem_limit_bytes=56_400_000
        ),
        name="forces",
    )(blocks, homes, others, homes.reshape(1, PAIRS), *tables)
    total_atoms = 4 * 16 * 16 * TILES * TILE
    short = short * (32.0 * 2.0 / math.sqrt(256.0))
    long = long * (-0.4 * NG / math.sqrt(NG * total_atoms))
    return short.reshape(3, 1, 1, TILES * TILE), long.reshape(3, 1, 1, TILES * TILE)


def solution(mesh):
    tables = make_tables()

    def whole(atoms, pair_home, pair_other):
        fixed = [jnp.asarray(tables[name]) for name in NAMES]
        mapped = jax.shard_map(
            lambda a, h, o: on_device(a, h, o, *fixed),
            mesh=mesh,
            in_specs=(P(None, "grp", "dom", "pen"), P("grp", "dom", "pen"), P("grp", "dom", "pen")),
            out_specs=(P(None, "grp", "dom", "pen"), P(None, "grp", "dom", "pen")),
            check_vma=False,
        )
        return mapped(atoms, pair_home, pair_other)

    return whole
```

```python
import functools
import math

import jax
import jax.numpy as jnp
import numpy as np
from jax import lax
from jax.experimental import pallas as pl
from jax.experimental.pallas import tpu as pltpu
from jax.sharding import PartitionSpec as P

NG = 128
TILE = 128
TILES = 32
PAIRS = 64
SIDE = 11
PEERS = 32
MESH = pl.DeviceIdType.MESH
f32 = jnp.float32
bf16 = jnp.bfloat16


def basis(cells):
    k = np.arange(NG)[:, None]
    m = np.where(k <= NG // 2, k, k - NG // 2)
    angle = 2.0 * np.pi * np.mod(m * cells[None, :], NG) / NG
    return np.where(k <= NG // 2, np.cos(angle), np.sin(angle))


def turning(starts, lanes, used):
    k = np.arange(NG)[:, None]
    m = np.where(k <= NG // 2, k, k - NG // 2)
    first = 2.0 * np.pi * np.mod(m * starts[None, :], NG) / NG
    second = 2.0 * np.pi * np.mod(m * lanes[None, :], NG) / NG
    is_cos = k <= NG // 2
    part_c = np.where(is_cos, np.cos(second), np.sin(second)) * used[None, :]
    part_s = np.where(is_cos, -np.sin(second), np.cos(second)) * used[None, :]
    return np.cos(first), np.sin(first), part_c, part_s


def halves(table):
    table = np.asarray(table, np.float32)
    high = table.astype(jnp.bfloat16)
    low = (table - high.astype(np.float32)).astype(jnp.bfloat16)
    return high, low


def spread_columns(turn_c, turn_s, inner):
    count = turn_c.shape[1]
    out = np.zeros((inner, 2, 16, count, inner))
    for i in range(inner):
        out[i, 0, :, :, i] = turn_c[:16]
        out[i, 1, :, :, i] = turn_s[:16]
    return out.reshape(inner * 32, count * inner)


def patch_places():
    places = [(x, y) for y in range(SIDE) for x in range(8)]
    places += [(x, y) for x in range(8, SIDE) for y in range(8)]
    places += [(x, y) for x in range(8, SIDE) for y in range(8, SIDE)]
    places += [(SIDE, SIDE)] * (NG - len(places))
    return np.array(places).T


def make_tables():
    row = np.arange(NG)
    row_x, row_y = patch_places()
    lane_z, lane_y = (row // 16) % 2, row % 16
    x_c, x_s, bx_c, bx_s = turning(8 * np.arange(16), row_x - 3, row < SIDE * SIDE)
    y_c, y_s, by_c, by_s = turning(8 * np.arange(8), 64 * lane_z - 3 + lane_y, lane_y < SIDE)
    x_cols, y_cols = spread_columns(x_c, x_s, 4), spread_columns(y_c, y_s, 4)
    xh, xl = halves(x_cols)
    yh, yl = halves(y_cols)
    forward_x = np.concatenate([xh, xh, xl], axis=1)
    forward_y = np.concatenate([yh, yh, yl], axis=1)
    inverse_x = np.concatenate([xh.T, xl.T], axis=0)
    inverse_y = np.concatenate([yh.T, yl.T], axis=0)
    pick_x = np.zeros((4, 2, NG, NG), np.float32)
    for j in range(4):
        for z in range(2):
            for r in range(SIDE * SIDE):
                pick_x[j, z, r, j * 32 + z * 16 + row_y[r]] = 1.0
    pick_y = np.zeros((4, NG, NG), np.float32)
    for i in range(4):
        for lane in range(NG):
            pick_y[i, lane, i * 4 + lane // 32] = 1.0
    zh, zl = halves(basis(row))
    return dict(
        forward_x=forward_x,
        forward_y=forward_y,
        inverse=np.concatenate([inverse_x, inverse_y], axis=0),
        picks=np.concatenate(
            [
                pick_x.reshape(1024, NG).astype(jnp.bfloat16),
                pick_y.reshape(512, NG).astype(jnp.bfloat16),
                zh,
                zl,
            ],
            axis=0,
        ),
        parts=np.concatenate([bx_c, bx_s, by_c, by_s], axis=0).astype(np.float32),
    )


NAMES = (
    "picks",
    "forward_x",
    "forward_y",
    "inverse",
    "parts",
)


def dot(a, b):
    return lax.dot_general(a, b, (((1,), (0,)), ((), ())), preferred_element_type=f32)


def dot_nt(a, b):
    return lax.dot_general(a, b, (((1,), (1,)), ((), ())), preferred_element_type=f32)


def split(x):
    high = x.astype(bf16)
    return high, (x - high.astype(f32)).astype(bf16)


def stacked(x):
    high = x.astype(bf16).astype(f32)
    return jnp.concatenate([high, x - high, high], axis=0).astype(bf16)


def spline_terms(scaled):
    floored = jnp.floor(scaled)
    w = scaled - floored
    remain = 1.0 - w
    sq = w * w
    cube = sq * w
    thetas = [
        remain * remain * remain * (1.0 / 6.0),
        (3.0 * cube - 6.0 * sq + 4.0) * (1.0 / 6.0),
        (-3.0 * cube + 3.0 * sq + 3.0 * w + 1.0) * (1.0 / 6.0),
        cube * (1.0 / 6.0),
    ]
    slopes = [
        -0.5 * remain * remain,
        1.5 * sq - 2.0 * w,
        -1.5 * sq + w + 0.5,
        0.5 * sq,
    ]
    return floored, thetas, slopes


def one_of(is_at, values):
    out = jnp.where(is_at[3], values[3], 0.0)
    for k in (2, 1, 0):
        out = jnp.where(is_at[k], values[k], out)
    return out


def matches(t):
    return [t == k for k in range(4)]


def unfolded(turned, n):
    rows = turned[32 * n : 32 * n + 16], turned[32 * n + 16 : 32 * n + 32]
    return tuple(jnp.concatenate([r] * (NG // 16), axis=0) for r in rows)


def folded(x):
    parts = [x[16 * k : 16 * k + 16] for k in range(NG // 16)]
    while len(parts) > 1:
        parts = [a + b for a, b in zip(parts[::2], parts[1::2])]
    return parts[0]


def turned_back(table, lines):
    high, low = split(jnp.concatenate(lines, axis=0))
    rows = table.shape[0] // 2
    full = dot(table, high)
    return full[:rows] + full[rows:] + dot(table[:rows], low)


def to_lines_x(got, forward_x, part_c, part_s, pick_x):
    both = jnp.concatenate([got[:64], got[64:]], axis=1)
    turned = dot(forward_x, stacked(both))
    c2, s2 = jnp.concatenate([part_c] * 2, axis=1), jnp.concatenate([part_s] * 2, axis=1)
    out = None
    for j in range(4):
        turn_c, turn_s = unfolded(turned, j)
        high, low = split(c2 * turn_c + s2 * turn_s)
        pick = pick_x[j * 256 : (j + 1) * 256]
        term = dot(high, pick) + dot(low, pick)
        out = term if out is None else out + term
    return out


def through_y(got, factor, forward_y, inverse_y, part_c, part_s, pick_y):
    total = (got[:32] + got[32:64]) + (got[64:96] + got[96:])
    turned = dot(forward_y, stacked(total))
    lines = []
    for i in range(4):
        turn_c, turn_s = unfolded(turned, i)
        lines.append(part_c * turn_c + part_s * turn_s)
    high, low = split(jnp.concatenate(lines, axis=1))
    freq = (dot(high, pick_y) + dot(low, pick_y)) * factor
    high, low = split(freq)
    wide = dot_nt(high, pick_y) + dot_nt(low, pick_y)
    lines = []
    for i in range(4):
        piece = wide[:, i * 128 : (i + 1) * 128]
        lines += [folded(part_c * piece), folded(part_s * piece)]
    return turned_back(inverse_y, lines)


def from_lines_x(got, inverse_x, part_c, part_s, pick_x):
    high, low = split(got)
    c2, s2 = jnp.concatenate([part_c] * 2, axis=1), jnp.concatenate([part_s] * 2, axis=1)
    lines = []
    for j in range(4):
        pick = pick_x[j * 256 : (j + 1) * 256]
        wide = dot_nt(high, pick) + dot_nt(low, pick)
        lines += [folded(c2 * wide), folded(s2 * wide)]
    out = turned_back(inverse_x, lines)
    return jnp.concatenate([out[:, :128], out[:, 128:]], axis=0)


def to_z(mesh, basis_z):
    high, low = split(mesh)
    full = dot(basis_z, high)
    return full[:128] + full[128:] + dot(basis_z[:128], low)


def from_z(got, basis_z):
    high, low = split(got.T)
    return dot(high, basis_z[:128]) + dot(high, basis_z[128:]) + dot(low, basis_z[:128])


def green_of(k_x, k_y, k_z):
    def mode(k):
        return jnp.where(k <= NG // 2, k, k - NG // 2)

    def weight(m):
        ratio = (2.0 + jnp.cos(m.astype(f32) * (2.0 * math.pi / NG))) / 3.0
        twice = jnp.where((m == 0) | (m == NG // 2), 1.0, 2.0)
        return twice / (ratio * ratio)

    m_x, m_y, m_z = mode(k_x), mode(k_y), mode(k_z)
    square = (m_x * m_x + m_z * m_z + m_y * m_y).astype(f32)
    beta = 0.6 * NG
    value = jnp.exp(square * (-math.pi * math.pi / (beta * beta)))
    value = value / (math.pi * jnp.maximum(square, 1.0))
    value = value * (weight(m_x) * weight(m_z)) * weight(m_y)
    return jnp.where(square > 0.5, value, 0.0)


def thirds(x):
    high = x.astype(bf16).astype(f32)
    rest = x - high
    middle = rest.astype(bf16).astype(f32)
    return high, middle, rest - middle


def pair_push(other, against):
    columns = jnp.concatenate([*thirds(other), jnp.ones_like(other)], axis=0).astype(bf16)
    wide = lax.dot_general(
        columns, against, (((0,), (0,)), ((), ())), preferred_element_type=f32
    )
    delta = [wide[:, 128 * c : 128 * c + 128] for c in range(3)]
    delta[2] = delta[2] - jnp.floor(delta[2] + 0.5)
    square = delta[0] * delta[0] + delta[1] * delta[1] + delta[2] * delta[2]
    weight = jnp.exp2(square * (-512.0 * math.log2(math.e))) * wide[:, 384:]
    return [jnp.sum(d * weight, axis=0, keepdims=True) for d in delta]


PLACE = 0
THETA = 12
SLOPE = 24
CHARGED = 36
Z_LOW = 40
FIELDS = 48


def kernel(
    atoms_hbm,
    home_hbm,
    other_hbm,
    home_row_hbm,
    picks_hbm,
    fx_hbm,
    fy_hbm,
    inverse_hbm,
    parts_hbm,
    short_ref,
    long_ref,
    home_smem,
    other_smem,
    home_vmem,
    near,
    fields,
    mesh,
    pushes,
    against,
    grads,
    pot_parts,
    z_table,
    xy_table,
    send_a,
    recv_a,
    send_b,
    recv_b,
    send_c,
    recv_c,
    send_d,
    recv_d,
    picks,
    forward_x,
    forward_y,
    inverse,
    parts,
    table_sems,
    atom_sem,
    send_sems,
    recv_sems,
    halo_send,
    halo_recv,
):
    grp = lax.axis_index("grp")
    dom = lax.axis_index("dom")
    pen = lax.axis_index("pen")
    z_hi, y_at = pen >> 3, pen & 7
    at_a = z_hi * 16 + dom
    at_b = grp * 8 + y_at

    def peer_a(k):
        t = (at_a + k) & (PEERS - 1)
        return t, {"grp": grp, "dom": t & 15, "pen": (t >> 4) * 8 + y_at}

    def peer_b(k):
        to_grp, to_y = (grp + (k >> 3)) & 3, (y_at + (k & 7)) & 7
        return to_grp * 8 + to_y, {"grp": to_grp, "dom": dom, "pen": z_hi * 8 + to_y}

    pen_next = {"grp": grp, "dom": dom, "pen": lax.rem(pen + 1, 16)}
    pen_prev = {"grp": grp, "dom": dom, "pen": lax.rem(pen + 15, 16)}
    dom_next = {"grp": grp, "dom": lax.rem(dom + 1, 16), "pen": pen}
    dom_prev = {"grp": grp, "dom": lax.rem(dom + 15, 16), "pen": pen}

    load_atoms = pltpu.make_async_copy(atoms_hbm, near.at[4], atom_sem)
    load_atoms.start()
    barrier = pltpu.get_barrier_semaphore()

    for n in range(1, PEERS):
        k = 16 + (n >> 1) * (1 if n & 1 else -1)
        pl.semaphore_signal(barrier, 1, device_id=peer_a(k)[1], device_id_type=MESH)
    for k in range(1, PEERS):
        pl.semaphore_signal(barrier, 1, device_id=peer_b(k)[1], device_id_type=MESH)
    pl.semaphore_signal(barrier, 1, device_id=pen_next, device_id_type=MESH)
    pl.semaphore_signal(barrier, 1, device_id=pen_prev, device_id_type=MESH)

    loads = [
        pltpu.make_async_copy(source, target, table_sems.at[n])
        for n, (source, target) in enumerate(
            (
                (picks_hbm, picks),
                (fx_hbm, forward_x),
                (fy_hbm, forward_y),
                (inverse_hbm, inverse),
                (parts_hbm, parts),
                (home_hbm, home_smem),
                (other_hbm, other_smem),
                (home_row_hbm, home_vmem),
            )
        )
    ]
    for load in loads:
        load.start()
    load_atoms.wait()

    charge = near[4, 3]
    for c, start in ((0, (dom * 8).astype(f32)), (1, (pen * 8).astype(f32)), (2, 3.0)):
        floored, thetas, slopes = spline_terms(near[4, c] * float(NG))
        lowest = floored - start
        for k in range(4):
            place = lowest + float(k)
            theta, slope = thetas[k], slopes[k]
            if c == 1:
                fields[CHARGED + k] = theta * charge
            if c == 2:
                place = jnp.where(place < 0.0, place + float(NG), place)
                high = theta.astype(bf16).astype(f32)
                fields[Z_LOW + k] = theta - high
                theta = high
                high = slope.astype(bf16).astype(f32)
                fields[Z_LOW + 4 + k] = slope - high
                slope = high
            fields[PLACE + 4 * c + k] = place
            fields[THETA + 4 * c + k] = theta
            fields[SLOPE + 4 * c + k] = slope

    z_at = lax.broadcasted_iota(jnp.int32, (NG, TILE), 0).astype(f32).astype(bf16)
    side_at = lax.broadcasted_iota(jnp.int32, (16, TILE), 0).astype(f32)
    corner_at = jnp.minimum(lax.broadcasted_iota(jnp.int32, (16, TILE), 0), 9).astype(f32)
    corner_x = jnp.floor((corner_at + 0.5) * (1.0 / 3.0))
    corner_y = 8.0 + corner_at - 3.0 * corner_x
    corner_x = corner_x + 8.0

    def row(field, tile):
        return fields[field, pl.ds(tile, 1), :]

    def rows_of(field, tile):
        return [row(field + k, tile) for k in range(4)]

    def narrow(field, tile):
        return [r.astype(bf16) for r in rows_of(field, tile)]

    def at_z(tile):
        return [z_at == r for r in narrow(PLACE + 8, tile)]

    def at(axis, where, tile):
        return [where == r for r in rows_of(PLACE + 4 * axis, tile)]

    def across(value, n):
        return jnp.broadcast_to(value[n : n + 1], (8, TILE))

    mesh[...] = jnp.zeros_like(mesh)

    def spread(step, carry):
        z_high, z_low, p_parts = [], [], []
        for n in range(4):
            tile = step * 4 + n
            is_z = at_z(tile)
            z_high.append(one_of(is_z, narrow(THETA + 8, tile)))
            z_low.append(one_of(is_z, narrow(Z_LOW, tile)))
            z_table[tile, :128, :128] = z_high[-1]
            z_table[tile, 128:, :128] = z_low[-1]
            t_x, t_y = rows_of(THETA, tile), rows_of(CHARGED, tile)
            w_x, w_y = one_of(at(0, side_at, tile), t_x), one_of(at(1, side_at, tile), t_y)
            pieces = [w_x[:8] * across(w_y, y) for y in range(SIDE)]
            pieces += [across(w_x, x) * w_y[:8] for x in range(8, SIDE)]
            pieces += [one_of(at(0, corner_x, tile), t_x) * one_of(at(1, corner_y, tile), t_y)]
            p_parts.append(split(jnp.concatenate(pieces, axis=0)))
        z_high = jnp.concatenate(z_high, axis=1)
        z_low = jnp.concatenate(z_low, axis=1)
        p_high = jnp.concatenate([p[0] for p in p_parts], axis=1)
        p_low = jnp.concatenate([p[1] for p in p_parts], axis=1)
        wide = dot_nt(z_high, jnp.concatenate([p_high, p_low], axis=0))
        mesh[...] += wide[:, :128] + wide[:, 128:] + dot_nt(z_low, p_high)
        return carry

    lax.fori_loop(0, TILES // 4, spread, 0, unroll=2)

    def put(ref, value):
        for n in range(value.shape[0] // 4):
            ref[n] = value[4 * n : 4 * n + 4]

    def taken(ref):
        return jnp.concatenate([ref[n] for n in range(PEERS)], axis=0)

    def exchange(source, target, phase, peer, own, slot, offset):
        def post(k, carry):
            index, device = peer(offset(k))
            pltpu.make_async_remote_copy(
                src_ref=source.at[slot(index)],
                dst_ref=target.at[own],
                send_sem=send_sems.at[phase],
                recv_sem=recv_sems.at[phase],
                device_id=device,
                device_id_type=MESH,
            ).start()
            return carry

        lax.fori_loop(0, PEERS - 1, post, 0)
        target[own] = source[slot(own)]

    def arrived(target, phase, device):
        whole = target.at[pl.ds(0, PEERS - 1)]
        both = pltpu.make_async_remote_copy(
            src_ref=whole,
            dst_ref=whole,
            send_sem=send_sems.at[phase],
            recv_sem=recv_sems.at[phase],
            device_id=device,
            device_id_type=MESH,
        )
        both.wait_recv()
        return both

    def same(index):
        return index

    def outward(n, middle):
        return middle + ((n + 1) >> 1) * (1 - 2 * (n & 1))

    def far_first(k):
        return outward(k, 16)

    def far_plane(k):
        return (outward(k & 3, 2) & 3) * 8 + (outward(k >> 2, 4) & 7)

    def low_first(k):
        return PEERS + k + (k >= at_a).astype(jnp.int32) - at_a

    loads[0].wait()
    put(send_a, to_z(mesh[...], picks[1536:]))
    pl.semaphore_wait(barrier, 2 * (PEERS - 1) + 2)
    exchange(send_a, recv_a, 0, peer_a, at_a, same, far_first)

    def halo(source, target, n, device):
        return pltpu.make_async_remote_copy(
            src_ref=near.at[source],
            dst_ref=near.at[target],
            send_sem=halo_send.at[n],
            recv_sem=halo_recv.at[n],
            device_id=device,
            device_id_type=MESH,
        )

    side = [halo(4, 3, 0, pen_next), halo(4, 5, 1, pen_prev)]
    pl.when(y_at != 7)(side[0].start)
    pl.when(y_at != 0)(side[1].start)
    ends = [
        halo(slot, slot - 3 if up else slot + 3, 2 + 2 * n + up, device)
        for n, slot in enumerate((3, 4, 5))
        for up, device in enumerate((dom_prev, dom_next))
    ]

    def hand_on(n):
        if n != 1:
            side[n // 2].wait_recv()
        for copy in ends[2 * n : 2 * n + 2]:
            copy.start()

    table_row = lax.broadcasted_iota(jnp.int32, (16, 4 * TILE), 0)
    table_block = lax.broadcasted_iota(jnp.int32, (16, 4 * TILE), 1) >> 7
    table_sign = jnp.where(table_block == 3, 1.0, -1.0)
    table_fixed = jnp.where(((table_row & 3) == table_block) & (table_row < 12), table_sign, 0.0)

    def home_table(tile, carry):
        rows = [near[4, c, pl.ds(tile, 1), :] for c in range(3)]
        filled = table_fixed
        parts_of = thirds(jnp.concatenate(rows + [jnp.zeros_like(rows[0])], axis=1))
        for k in range(3):
            filled = jnp.where(table_row == 12 + k, parts_of[k], filled)
        against[tile] = filled.astype(bf16)
        return carry

    lax.fori_loop(0, TILES, home_table, 0, unroll=2)

    def prepare(step, carry):
        for n in range(2):
            tile = step * 2 + n
            is_z = at_z(tile)
            z_table[tile, :128, 128:] = one_of(is_z, narrow(SLOPE + 8, tile))
            z_table[tile, 128:, 128:] = one_of(is_z, narrow(Z_LOW + 4, tile))
            t_x, d_x = rows_of(THETA, tile), rows_of(SLOPE, tile)
            t_y, d_y = rows_of(THETA + 4, tile), rows_of(SLOPE + 4, tile)
            is_x, is_y = at(0, side_at, tile), at(1, side_at, tile)
            xy_table[tile, 0:16] = one_of(is_x, t_x)
            xy_table[tile, 16:32] = one_of(is_x, d_x)
            xy_table[tile, 32:48] = one_of(is_y, t_y)
            xy_table[tile, 48:64] = one_of(is_y, d_y)
            is_x, is_y = at(0, corner_x, tile), at(1, corner_y, tile)
            cw_x, cs_x = one_of(is_x, t_x), one_of(is_x, d_x)
            cw_y, cs_y = one_of(is_y, t_y), one_of(is_y, d_y)
            xy_table[tile, 64:80] = cs_x * cw_y
            xy_table[tile, 80:96] = cw_x * cs_y
            xy_table[tile, 96:112] = cw_x * cw_y
        return carry

    lax.fori_loop(0, TILES // 2, prepare, 0)

    pl.delay(1000)
    pl.when(y_at == 7)(side[0].start)
    pl.when(y_at == 0)(side[1].start)

    for load in loads[1:]:
        load.wait()
    part_xc, part_xs, part_yc, part_ys = (parts[128 * n : 128 * n + 128, :] for n in range(4))
    lane = lax.broadcasted_iota(jnp.int32, (1, NG), 1)
    k_x = at_b * 4 + (lane // 4)
    k_z = at_a * 4 + lax.rem(lane, 4)
    k_y = lax.broadcasted_iota(jnp.int32, (NG, 1), 0)
    used = lane < 16
    factor = green_of(jnp.where(used, k_x, 1), k_y, jnp.where(used, k_z, 1))

    peer_one_a = peer_a(1)[1]
    peer_one_b = peer_b(1)[1]
    sent_0 = arrived(recv_a, 0, peer_one_a)
    put(send_b, to_lines_x(taken(recv_a), forward_x[...], part_xc, part_xs, picks[:1024]))
    exchange(send_b, recv_b, 1, peer_b, at_b, same, far_plane)
    hand_on(1)
    pl.when(y_at != 0)(lambda: hand_on(0))
    pl.when(y_at != 7)(lambda: hand_on(2))

    sent_1 = arrived(recv_b, 1, peer_one_b)
    put(
        send_c,
        through_y(
            taken(recv_b),
            factor,
            forward_y[...],
            inverse[128:],
            part_yc,
            part_ys,
            picks[1024:1536],
        ),
    )
    exchange(send_c, recv_c, 2, peer_b, at_b, lambda index: index & 7, far_plane)

    pl.when(y_at == 0)(lambda: hand_on(0))
    pl.when(y_at == 7)(lambda: hand_on(2))

    sent_2 = arrived(recv_c, 2, peer_one_b)
    put(send_d, from_lines_x(taken(recv_c), inverse[:128], part_xc, part_xs, picks[:1024]))
    exchange(send_d, recv_d, 3, peer_a, at_a, same, low_first)

    for copy in ends:
        copy.wait()
    for copy in side:
        copy.wait_send()
    def period(step, at_edge):
        below = (step == -1) & (at_edge == 0)
        above = (step == 1) & (at_edge == 15)
        return jnp.where(below, 1.0, jnp.where(above, -1.0, 0.0)).astype(f32)

    def pair(n, carry):
        home, other = home_smem[n], other_smem[n]
        block, tile = other >> 5, other & 31
        step_d = jnp.where(block < 3, -1, jnp.where(block < 6, 0, 1))
        step_p = block - 3 * (step_d + 1) - 1
        far = [near[block, c, pl.ds(tile, 1), :] for c in range(4)]
        far[0] = far[0] - period(step_d, dom)
        far[1] = far[1] - period(step_p, pen)
        rows = pair_push(jnp.concatenate(far, axis=0), against[home])
        for c in range(3):
            pushes[c, pl.ds(n, 1), :] = rows[c]
        return carry

    lax.fori_loop(0, PAIRS, pair, 0, unroll=4)
    tile_ids = lax.broadcasted_iota(jnp.int32, (TILES, PAIRS), 0)
    owners = jnp.where(home_vmem[...] == tile_ids, 1.0, 0.0).astype(bf16)
    for c in range(3):
        high, low = split(pushes[c])
        short_ref[c] = (dot(owners, high) + dot(owners, low)) * charge

    sent_3 = arrived(recv_d, 3, peer_one_a)
    pot_high, pot_low = split(from_z(taken(recv_d), picks[1536:]))
    for n in range(2):
        pot_parts[:128, 128 * n : 128 * n + 128] = pot_high
        pot_parts[128:, 128 * n : 128 * n + 128] = pot_low

    def interpolate(step, carry):
        for n in range(2):
            tile = step * 2 + n
            wide = dot(pot_parts[...], z_table[tile])
            along = wide[:128] + wide[128:]
            value = [along[8 * k : 8 * k + 8, :128] for k in range(16)]
            slope = [along[8 * k : 8 * k + 8, 128:] for k in range(16)]
            w_x, s_x, w_y, s_y = (xy_table[tile, 16 * k : 16 * k + 16] for k in range(4))
            by_y = [[], [], []]
            for y in range(SIDE):
                by_y[0].append(across(w_y, y) * value[y])
                by_y[1].append(across(s_y, y) * value[y])
                by_y[2].append(across(w_y, y) * slope[y])
            by_x = [[], [], []]
            for x in range(8, SIDE):
                by_x[0].append(across(s_x, x) * value[x + 3])
                by_x[1].append(across(w_x, x) * value[x + 3])
                by_x[2].append(across(w_x, x) * slope[x + 3])
            ends_x, ends_y = (s_x, w_x, w_x), (w_y, s_y, w_y)
            for c in range(3):
                total = ends_x[c][:8] * sum(by_y[c][1:], by_y[c][0])
                total += ends_y[c][:8] * sum(by_x[c][1:], by_x[c][0])
                own = slope if c == 2 else value
                corner = xy_table[tile, 64 + 16 * c : 80 + 16 * c]
                total += corner[:8] * own[14] + corner[8:] * own[15]
                grads[c, pl.ds(tile, 1), :] = jnp.sum(total, axis=0, keepdims=True)
        return carry

    lax.fori_loop(0, TILES // 2, interpolate, 0, unroll=4)
    for sent in (sent_0, sent_1, sent_2, sent_3):
        sent.wait_send()
    for c in range(3):
        long_ref[c] = grads[c] * charge


def on_device(atoms, pair_home, pair_other, *tables):
    hbm = pl.BlockSpec(memory_space=pl.ANY)
    vmem = pl.BlockSpec(memory_space=pltpu.VMEM)
    blocks = atoms.reshape(4, TILES, TILE)
    homes = pair_home.reshape(PAIRS)
    others = pair_other.reshape(PAIRS)
    force = jax.ShapeDtypeStruct((3, TILES, TILE), f32)
    message = pltpu.VMEM((PEERS, 4, NG), f32)
    short, long = pl.pallas_call(
        kernel,
        out_shape=(force, force),
        in_specs=[hbm] * (4 + len(NAMES)),
        out_specs=(vmem, vmem),
        scratch_shapes=[
            pltpu.SMEM((PAIRS,), jnp.int32),
            pltpu.SMEM((PAIRS,), jnp.int32),
            pltpu.VMEM((1, PAIRS), jnp.int32),
            pltpu.VMEM((9, 4, TILES, TILE), f32),
            pltpu.VMEM((FIELDS, TILES, TILE), f32),
            pltpu.VMEM((NG, NG), f32),
            pltpu.VMEM((3, PAIRS, TILE), f32),
            pltpu.VMEM((TILES, 16, 4 * TILE), bf16),
            pltpu.VMEM((3, TILES, TILE), f32),
            pltpu.VMEM((2 * NG, 2 * NG), bf16),
            pltpu.VMEM((TILES, 2 * NG, 2 * TILE), bf16),
            pltpu.VMEM((TILES, 112, TILE), f32),
            message,
            message,
            message,
            message,
            pltpu.VMEM((8, 4, NG), f32),
            message,
            message,
            message,
            *[pltpu.VMEM(t.shape, t.dtype) for t in tables],
            pltpu.SemaphoreType.DMA((len(NAMES) + 3,)),
            pltpu.SemaphoreType.DMA,
            pltpu.SemaphoreType.DMA((4,)),
            pltpu.SemaphoreType.DMA((4,)),
            pltpu.SemaphoreType.DMA((8,)),
            pltpu.SemaphoreType.DMA((8,)),
        ],
        compiler_params=pltpu.CompilerParams(
            collective_id=0, has_side_effects=True, vmem_limit_bytes=48 << 20
        ),
        name="forces",
    )(
        *(
            pltpu.with_memory_space_constraint(operand, pltpu.HBM)
            for operand in (blocks, homes, others, homes.reshape(1, PAIRS), *tables)
        )
    )
    total_atoms = 4 * 16 * 16 * TILES * TILE
    short = short * (32.0 * 2.0 / math.sqrt(256.0))
    long = long * (-0.4 * NG / math.sqrt(NG * total_atoms))
    return short.reshape(3, 1, 1, TILES * TILE), long.reshape(3, 1, 1, TILES * TILE)


def solution(mesh):
    tables = make_tables()

    def whole(atoms, pair_home, pair_other):
        fixed = [jnp.asarray(tables[name]) for name in NAMES]
        mapped = jax.shard_map(
            lambda a, h, o: on_device(a, h, o, *fixed),
            mesh=mesh,
            in_specs=(P(None, "grp", "dom", "pen"), P("grp", "dom", "pen"), P("grp", "dom", "pen")),
            out_specs=(P(None, "grp", "dom", "pen"), P(None, "grp", "dom", "pen")),
            check_vma=False,
        )
        return mapped(atoms, pair_home, pair_other)

    return whole
```

```python
import functools
import math

import jax
import jax.numpy as jnp
import numpy as np
from jax import lax
from jax.experimental import pallas as pl
from jax.experimental.pallas import tpu as pltpu
from jax.sharding import PartitionSpec as P

NG = 128
TILE = 128
TILES = 32
PAIRS = 64
SIDE = 11
PEERS = 32
MESH = pl.DeviceIdType.MESH
f32 = jnp.float32
bf16 = jnp.bfloat16


def basis(cells):
    k = np.arange(NG)[:, None]
    m = np.where(k <= NG // 2, k, k - NG // 2)
    angle = 2.0 * np.pi * np.mod(m * cells[None, :], NG) / NG
    return np.where(k <= NG // 2, np.cos(angle), np.sin(angle))


def turning(starts, lanes, used):
    k = np.arange(NG)[:, None]
    m = np.where(k <= NG // 2, k, k - NG // 2)
    first = 2.0 * np.pi * np.mod(m * starts[None, :], NG) / NG
    second = 2.0 * np.pi * np.mod(m * lanes[None, :], NG) / NG
    is_cos = k <= NG // 2
    part_c = np.where(is_cos, np.cos(second), np.sin(second)) * used[None, :]
    part_s = np.where(is_cos, -np.sin(second), np.cos(second)) * used[None, :]
    return np.cos(first), np.sin(first), part_c, part_s


def halves(table):
    table = np.asarray(table, np.float32)
    high = table.astype(jnp.bfloat16)
    low = (table - high.astype(np.float32)).astype(jnp.bfloat16)
    return high, low


def spread_columns(turn_c, turn_s, inner):
    count = turn_c.shape[1]
    out = np.zeros((inner, 2, 16, count, inner))
    for i in range(inner):
        out[i, 0, :, :, i] = turn_c[:16]
        out[i, 1, :, :, i] = turn_s[:16]
    return out.reshape(inner * 32, count * inner)


def patch_places():
    places = [(x, y) for y in range(SIDE) for x in range(8)]
    places += [(x, y) for x in range(8, SIDE) for y in range(8)]
    places += [(x, y) for x in range(8, SIDE) for y in range(8, SIDE)]
    places += [(SIDE, SIDE)] * (NG - len(places))
    return np.array(places).T


def make_tables():
    row = np.arange(NG)
    row_x, row_y = patch_places()
    lane_z, lane_y = (row // 16) % 2, row % 16
    x_c, x_s, bx_c, bx_s = turning(8 * np.arange(16), row_x - 3, row < SIDE * SIDE)
    y_c, y_s, by_c, by_s = turning(8 * np.arange(8), 64 * lane_z - 3 + lane_y, lane_y < SIDE)
    x_cols, y_cols = spread_columns(x_c, x_s, 4), spread_columns(y_c, y_s, 4)
    xh, xl = halves(x_cols)
    yh, yl = halves(y_cols)
    forward_x = np.concatenate([xh, xh, xl], axis=1)
    forward_y = np.concatenate([yh, yh, yl], axis=1)
    inverse_x = np.concatenate([xh.T, xl.T], axis=0)
    inverse_y = np.concatenate([yh.T, yl.T], axis=0)
    pick_x = np.zeros((4, 2, NG, NG), np.float32)
    for j in range(4):
        for z in range(2):
            for r in range(SIDE * SIDE):
                pick_x[j, z, r, j * 32 + z * 16 + row_y[r]] = 1.0
    pick_y = np.zeros((4, NG, NG), np.float32)
    for i in range(4):
        for lane in range(NG):
            pick_y[i, lane, i * 4 + lane // 32] = 1.0
    zh, zl = halves(basis(row))
    return dict(
        forward_x=forward_x,
        forward_y=forward_y,
        inverse=np.concatenate([inverse_x, inverse_y], axis=0),
        picks=np.concatenate(
            [
                pick_x.reshape(1024, NG).astype(jnp.bfloat16),
                pick_y.reshape(512, NG).astype(jnp.bfloat16),
                zh,
                zl,
            ],
            axis=0,
        ),
        parts=np.concatenate([bx_c, bx_s, by_c, by_s], axis=0).astype(np.float32),
    )


NAMES = (
    "picks",
    "forward_x",
    "forward_y",
    "inverse",
    "parts",
)


def dot(a, b):
    return lax.dot_general(a, b, (((1,), (0,)), ((), ())), preferred_element_type=f32)


def dot_nt(a, b):
    return lax.dot_general(a, b, (((1,), (1,)), ((), ())), preferred_element_type=f32)


def split(x):
    high = x.astype(bf16)
    return high, (x - high.astype(f32)).astype(bf16)


def stacked(x):
    high = x.astype(bf16).astype(f32)
    return jnp.concatenate([high, x - high, high], axis=0).astype(bf16)


def spline_terms(scaled):
    floored = jnp.floor(scaled)
    w = scaled - floored
    remain = 1.0 - w
    sq = w * w
    cube = sq * w
    thetas = [
        remain * remain * remain * (1.0 / 6.0),
        (3.0 * cube - 6.0 * sq + 4.0) * (1.0 / 6.0),
        (-3.0 * cube + 3.0 * sq + 3.0 * w + 1.0) * (1.0 / 6.0),
        cube * (1.0 / 6.0),
    ]
    slopes = [
        -0.5 * remain * remain,
        1.5 * sq - 2.0 * w,
        -1.5 * sq + w + 0.5,
        0.5 * sq,
    ]
    return floored, thetas, slopes


def one_of(is_at, values):
    out = jnp.where(is_at[3], values[3], 0.0)
    for k in (2, 1, 0):
        out = jnp.where(is_at[k], values[k], out)
    return out


def matches(t):
    return [t == k for k in range(4)]


def unfolded(turned, n):
    rows = turned[32 * n : 32 * n + 16], turned[32 * n + 16 : 32 * n + 32]
    return tuple(jnp.concatenate([r] * (NG // 16), axis=0) for r in rows)


def folded(x):
    parts = [x[16 * k : 16 * k + 16] for k in range(NG // 16)]
    while len(parts) > 1:
        parts = [a + b for a, b in zip(parts[::2], parts[1::2])]
    return parts[0]


def turned_back(table, lines):
    high, low = split(jnp.concatenate(lines, axis=0))
    rows = table.shape[0] // 2
    full = dot(table, high)
    return full[:rows] + full[rows:] + dot(table[:rows], low)


def to_lines_x(got, forward_x, part_c, part_s, pick_x):
    both = jnp.concatenate([got[:64], got[64:]], axis=1)
    turned = dot(forward_x, stacked(both))
    c2, s2 = jnp.concatenate([part_c] * 2, axis=1), jnp.concatenate([part_s] * 2, axis=1)
    out = None
    for j in range(4):
        turn_c, turn_s = unfolded(turned, j)
        high, low = split(c2 * turn_c + s2 * turn_s)
        pick = pick_x[j * 256 : (j + 1) * 256]
        term = dot(high, pick) + dot(low, pick)
        out = term if out is None else out + term
    return out


def through_y(got, factor, forward_y, inverse_y, part_c, part_s, pick_y):
    total = (got[:32] + got[32:64]) + (got[64:96] + got[96:])
    turned = dot(forward_y, stacked(total))
    lines = []
    for i in range(4):
        turn_c, turn_s = unfolded(turned, i)
        lines.append(part_c * turn_c + part_s * turn_s)
    high, low = split(jnp.concatenate(lines, axis=1))
    freq = (dot(high, pick_y) + dot(low, pick_y)) * factor
    high, low = split(freq)
    wide = dot_nt(high, pick_y) + dot_nt(low, pick_y)
    lines = []
    for i in range(4):
        piece = wide[:, i * 128 : (i + 1) * 128]
        lines += [folded(part_c * piece), folded(part_s * piece)]
    return turned_back(inverse_y, lines)


def from_lines_x(got, inverse_x, part_c, part_s, pick_x):
    high, low = split(got)
    c2, s2 = jnp.concatenate([part_c] * 2, axis=1), jnp.concatenate([part_s] * 2, axis=1)
    lines = []
    for j in range(4):
        pick = pick_x[j * 256 : (j + 1) * 256]
        wide = dot_nt(high, pick) + dot_nt(low, pick)
        lines += [folded(c2 * wide), folded(s2 * wide)]
    out = turned_back(inverse_x, lines)
    return jnp.concatenate([out[:, :128], out[:, 128:]], axis=0)


def to_z(mesh, basis_z):
    high, low = split(mesh)
    full = dot(basis_z, high)
    return full[:128] + full[128:] + dot(basis_z[:128], low)


def from_z(got, basis_z):
    high, low = split(got.T)
    return dot(high, basis_z[:128]) + dot(high, basis_z[128:]) + dot(low, basis_z[:128])


def green_of(k_x, k_y, k_z):
    def mode(k):
        return jnp.where(k <= NG // 2, k, k - NG // 2)

    def weight(m):
        ratio = (2.0 + jnp.cos(m.astype(f32) * (2.0 * math.pi / NG))) / 3.0
        twice = jnp.where((m == 0) | (m == NG // 2), 1.0, 2.0)
        return twice / (ratio * ratio)

    m_x, m_y, m_z = mode(k_x), mode(k_y), mode(k_z)
    square = (m_x * m_x + m_z * m_z + m_y * m_y).astype(f32)
    beta = 0.6 * NG
    value = jnp.exp(square * (-math.pi * math.pi / (beta * beta)))
    value = value / (math.pi * jnp.maximum(square, 1.0))
    value = value * (weight(m_x) * weight(m_z)) * weight(m_y)
    return jnp.where(square > 0.5, value, 0.0)


def thirds(x):
    high = x.astype(bf16).astype(f32)
    rest = x - high
    middle = rest.astype(bf16).astype(f32)
    return high, middle, rest - middle


def pair_push(other, against):
    columns = jnp.concatenate([*thirds(other), jnp.ones_like(other)], axis=0).astype(bf16)
    wide = lax.dot_general(
        columns, against, (((0,), (0,)), ((), ())), preferred_element_type=f32
    )
    delta = [wide[:, 128 * c : 128 * c + 128] for c in range(3)]
    delta[2] = delta[2] - jnp.floor(delta[2] + 0.5)
    square = delta[0] * delta[0] + delta[1] * delta[1] + delta[2] * delta[2]
    weight = jnp.exp2(square * (-512.0 * math.log2(math.e))) * wide[:, 384:]
    return [jnp.sum(d * weight, axis=0, keepdims=True) for d in delta]


PLACE = 0
THETA = 12
SLOPE = 24
CHARGED = 36
Z_LOW = 40
FIELDS = 48


def kernel(
    atoms_hbm,
    home_hbm,
    other_hbm,
    home_row_hbm,
    picks_hbm,
    fx_hbm,
    fy_hbm,
    inverse_hbm,
    parts_hbm,
    short_ref,
    long_ref,
    home_smem,
    other_smem,
    home_vmem,
    near,
    fields,
    mesh,
    pushes,
    against,
    grads,
    pot_parts,
    z_table,
    xy_table,
    send_a,
    recv_a,
    send_b,
    recv_b,
    send_c,
    recv_c,
    send_d,
    recv_d,
    picks,
    forward_x,
    forward_y,
    inverse,
    parts,
    table_sems,
    atom_sem,
    send_sems,
    recv_sems,
    halo_send,
    halo_recv,
):
    grp = lax.axis_index("grp")
    dom = lax.axis_index("dom")
    pen = lax.axis_index("pen")
    z_hi, y_at = pen >> 3, pen & 7
    at_a = z_hi * 16 + dom
    at_b = grp * 8 + y_at

    def peer_a(k):
        t = (at_a + k) & (PEERS - 1)
        return t, {"grp": grp, "dom": t & 15, "pen": (t >> 4) * 8 + y_at}

    def peer_b(k):
        to_grp, to_y = (grp + (k >> 3)) & 3, (y_at + (k & 7)) & 7
        return to_grp * 8 + to_y, {"grp": to_grp, "dom": dom, "pen": z_hi * 8 + to_y}

    pen_next = {"grp": grp, "dom": dom, "pen": lax.rem(pen + 1, 16)}
    pen_prev = {"grp": grp, "dom": dom, "pen": lax.rem(pen + 15, 16)}
    dom_next = {"grp": grp, "dom": lax.rem(dom + 1, 16), "pen": pen}
    dom_prev = {"grp": grp, "dom": lax.rem(dom + 15, 16), "pen": pen}

    load_atoms = pltpu.make_async_copy(atoms_hbm, near.at[4], atom_sem)
    load_atoms.start()
    barrier = pltpu.get_barrier_semaphore()

    def outward(n, middle):
        return middle + ((n + 1) >> 1) * (1 - 2 * (n & 1))

    def far_first(k):
        return outward(k, 16)

    def far_plane(k):
        return (outward(k & 3, 2) & 3) * 8 + (outward(k >> 2, 4) & 7)

    pl.semaphore_signal(barrier, 1, device_id=pen_next, device_id_type=MESH)
    pl.semaphore_signal(barrier, 1, device_id=pen_prev, device_id_type=MESH)
    for n in range(PEERS - 1):
        pl.semaphore_signal(barrier, 1, device_id=peer_a(far_first(n))[1], device_id_type=MESH)
        pl.semaphore_signal(barrier, 1, device_id=peer_b(far_plane(n))[1], device_id_type=MESH)

    loads = [
        pltpu.make_async_copy(source, target, table_sems.at[n])
        for n, (source, target) in enumerate(
            (
                (picks_hbm, picks),
                (fx_hbm, forward_x),
                (fy_hbm, forward_y),
                (inverse_hbm, inverse),
                (parts_hbm, parts),
                (home_hbm, home_smem),
                (other_hbm, other_smem),
                (home_row_hbm, home_vmem),
            )
        )
    ]
    for load in loads:
        load.start()
    load_atoms.wait()

    charge = near[4, 3]
    for c, start in ((0, (dom * 8).astype(f32)), (1, (pen * 8).astype(f32)), (2, 3.0)):
        floored, thetas, slopes = spline_terms(near[4, c] * float(NG))
        lowest = floored - start
        for k in range(4):
            place = lowest + float(k)
            theta, slope = thetas[k], slopes[k]
            if c == 1:
                fields[CHARGED + k] = theta * charge
            if c == 2:
                place = jnp.where(place < 0.0, place + float(NG), place)
                high = theta.astype(bf16).astype(f32)
                fields[Z_LOW + k] = theta - high
                theta = high
                high = slope.astype(bf16).astype(f32)
                fields[Z_LOW + 4 + k] = slope - high
                slope = high
            fields[PLACE + 4 * c + k] = place
            fields[THETA + 4 * c + k] = theta
            fields[SLOPE + 4 * c + k] = slope

    z_at = lax.broadcasted_iota(jnp.int32, (NG, TILE), 0).astype(f32).astype(bf16)
    side_at = lax.broadcasted_iota(jnp.int32, (16, TILE), 0).astype(f32)
    corner_at = jnp.minimum(lax.broadcasted_iota(jnp.int32, (16, TILE), 0), 9).astype(f32)
    corner_x = jnp.floor((corner_at + 0.5) * (1.0 / 3.0))
    corner_y = 8.0 + corner_at - 3.0 * corner_x
    corner_x = corner_x + 8.0

    def row(field, tile):
        return fields[field, pl.ds(tile, 1), :]

    def rows_of(field, tile):
        return [row(field + k, tile) for k in range(4)]

    def narrow(field, tile):
        return [r.astype(bf16) for r in rows_of(field, tile)]

    def at_z(tile):
        return [z_at == r for r in narrow(PLACE + 8, tile)]

    def at(axis, where, tile):
        return [where == r for r in rows_of(PLACE + 4 * axis, tile)]

    def across(value, n):
        return jnp.broadcast_to(value[n : n + 1], (8, TILE))

    mesh[...] = jnp.zeros_like(mesh)

    def spread(step, carry):
        z_high, z_low, p_parts = [], [], []
        for n in range(4):
            tile = step * 4 + n
            is_z = at_z(tile)
            z_high.append(one_of(is_z, narrow(THETA + 8, tile)))
            z_low.append(one_of(is_z, narrow(Z_LOW, tile)))
            z_table[tile, :128, :128] = z_high[-1]
            z_table[tile, 128:, :128] = z_low[-1]
            t_x, t_y = rows_of(THETA, tile), rows_of(CHARGED, tile)
            w_x, w_y = one_of(at(0, side_at, tile), t_x), one_of(at(1, side_at, tile), t_y)
            pieces = [w_x[:8] * across(w_y, y) for y in range(SIDE)]
            pieces += [across(w_x, x) * w_y[:8] for x in range(8, SIDE)]
            pieces += [one_of(at(0, corner_x, tile), t_x) * one_of(at(1, corner_y, tile), t_y)]
            p_parts.append(split(jnp.concatenate(pieces, axis=0)))
        z_high = jnp.concatenate(z_high, axis=1)
        z_low = jnp.concatenate(z_low, axis=1)
        p_high = jnp.concatenate([p[0] for p in p_parts], axis=1)
        p_low = jnp.concatenate([p[1] for p in p_parts], axis=1)
        wide = dot_nt(z_high, jnp.concatenate([p_high, p_low], axis=0))
        mesh[...] += wide[:, :128] + wide[:, 128:] + dot_nt(z_low, p_high)
        return carry

    lax.fori_loop(0, TILES // 4, spread, 0, unroll=4)

    def put(ref, value):
        for n in range(value.shape[0] // 4):
            ref[n] = value[4 * n : 4 * n + 4]

    def taken(ref):
        return jnp.concatenate([ref[n] for n in range(PEERS)], axis=0)

    def exchange(source, target, phase, peer, own, slot, offset):
        def post(k, carry):
            index, device = peer(offset(k))
            pltpu.make_async_remote_copy(
                src_ref=source.at[slot(index)],
                dst_ref=target.at[own],
                send_sem=send_sems.at[phase],
                recv_sem=recv_sems.at[phase],
                device_id=device,
                device_id_type=MESH,
            ).start()
            return carry

        lax.fori_loop(0, PEERS - 1, post, 0)
        target[own] = source[slot(own)]

    def arrived(target, phase, device):
        whole = target.at[pl.ds(0, PEERS - 1)]
        both = pltpu.make_async_remote_copy(
            src_ref=whole,
            dst_ref=whole,
            send_sem=send_sems.at[phase],
            recv_sem=recv_sems.at[phase],
            device_id=device,
            device_id_type=MESH,
        )
        both.wait_recv()
        return both

    def same(index):
        return index

    def low_first(k):
        return PEERS + k + (k >= at_a).astype(jnp.int32) - at_a

    loads[0].wait()
    put(send_a, to_z(mesh[...], picks[1536:]))
    pl.semaphore_wait(barrier, 2 * (PEERS - 1) + 2)
    exchange(send_a, recv_a, 0, peer_a, at_a, same, far_first)

    def halo(source, target, n, device):
        return pltpu.make_async_remote_copy(
            src_ref=near.at[source],
            dst_ref=near.at[target],
            send_sem=halo_send.at[n],
            recv_sem=halo_recv.at[n],
            device_id=device,
            device_id_type=MESH,
        )

    side = [halo(4, 3, 0, pen_next), halo(4, 5, 1, pen_prev)]
    pl.when(y_at != 7)(side[0].start)
    pl.when(y_at != 0)(side[1].start)
    ends = [
        halo(slot, slot - 3 if up else slot + 3, 2 + 2 * n + up, device)
        for n, slot in enumerate((3, 4, 5))
        for up, device in enumerate((dom_prev, dom_next))
    ]

    def hand_on(n):
        if n != 1:
            side[n // 2].wait_recv()
        for copy in ends[2 * n : 2 * n + 2]:
            copy.start()

    table_row = lax.broadcasted_iota(jnp.int32, (16, 4 * TILE), 0)
    table_block = lax.broadcasted_iota(jnp.int32, (16, 4 * TILE), 1) >> 7
    table_sign = jnp.where(table_block == 3, 1.0, -1.0)
    table_fixed = jnp.where(((table_row & 3) == table_block) & (table_row < 12), table_sign, 0.0)

    def home_table(tile, carry):
        rows = [near[4, c, pl.ds(tile, 1), :] for c in range(3)]
        filled = table_fixed
        parts_of = thirds(jnp.concatenate(rows + [jnp.zeros_like(rows[0])], axis=1))
        for k in range(3):
            filled = jnp.where(table_row == 12 + k, parts_of[k], filled)
        against[tile] = filled.astype(bf16)
        return carry

    lax.fori_loop(0, TILES, home_table, 0, unroll=2)

    def prepare(step, carry):
        for n in range(2):
            tile = step * 2 + n
            is_z = at_z(tile)
            z_table[tile, :128, 128:] = one_of(is_z, narrow(SLOPE + 8, tile))
            z_table[tile, 128:, 128:] = one_of(is_z, narrow(Z_LOW + 4, tile))
            t_x, d_x = rows_of(THETA, tile), rows_of(SLOPE, tile)
            t_y, d_y = rows_of(THETA + 4, tile), rows_of(SLOPE + 4, tile)
            is_x, is_y = at(0, side_at, tile), at(1, side_at, tile)
            xy_table[tile, 0:16] = one_of(is_x, t_x)
            xy_table[tile, 16:32] = one_of(is_x, d_x)
            xy_table[tile, 32:48] = one_of(is_y, t_y)
            xy_table[tile, 48:64] = one_of(is_y, d_y)
            is_x, is_y = at(0, corner_x, tile), at(1, corner_y, tile)
            cw_x, cs_x = one_of(is_x, t_x), one_of(is_x, d_x)
            cw_y, cs_y = one_of(is_y, t_y), one_of(is_y, d_y)
            xy_table[tile, 64:80] = cs_x * cw_y
            xy_table[tile, 80:96] = cw_x * cs_y
            xy_table[tile, 96:112] = cw_x * cw_y
        return carry

    lax.fori_loop(0, TILES // 2, prepare, 0)

    pl.delay(1000)
    pl.when(y_at == 7)(side[0].start)
    pl.when(y_at == 0)(side[1].start)

    for load in loads[1:]:
        load.wait()
    part_xc, part_xs, part_yc, part_ys = (parts[128 * n : 128 * n + 128, :] for n in range(4))
    lane = lax.broadcasted_iota(jnp.int32, (1, NG), 1)
    k_x = at_b * 4 + (lane // 4)
    k_z = at_a * 4 + lax.rem(lane, 4)
    k_y = lax.broadcasted_iota(jnp.int32, (NG, 1), 0)
    used = lane < 16
    factor = green_of(jnp.where(used, k_x, 1), k_y, jnp.where(used, k_z, 1))

    peer_one_a = peer_a(1)[1]
    peer_one_b = peer_b(1)[1]
    sent_0 = arrived(recv_a, 0, peer_one_a)
    put(send_b, to_lines_x(taken(recv_a), forward_x[...], part_xc, part_xs, picks[:1024]))
    exchange(send_b, recv_b, 1, peer_b, at_b, same, far_plane)
    hand_on(1)
    pl.when(y_at != 0)(lambda: hand_on(0))
    pl.when(y_at != 7)(lambda: hand_on(2))

    sent_1 = arrived(recv_b, 1, peer_one_b)
    put(
        send_c,
        through_y(
            taken(recv_b),
            factor,
            forward_y[...],
            inverse[128:],
            part_yc,
            part_ys,
            picks[1024:1536],
        ),
    )
    exchange(send_c, recv_c, 2, peer_b, at_b, lambda index: index & 7, far_plane)

    pl.when(y_at == 0)(lambda: hand_on(0))
    pl.when(y_at == 7)(lambda: hand_on(2))

    sent_2 = arrived(recv_c, 2, peer_one_b)
    put(send_d, from_lines_x(taken(recv_c), inverse[:128], part_xc, part_xs, picks[:1024]))
    exchange(send_d, recv_d, 3, peer_a, at_a, same, low_first)

    for copy in ends:
        copy.wait()
    for copy in side:
        copy.wait_send()
    def period(step, at_edge):
        below = (step == -1) & (at_edge == 0)
        above = (step == 1) & (at_edge == 15)
        return jnp.where(below, 1.0, jnp.where(above, -1.0, 0.0)).astype(f32)

    def pair(n, carry):
        home, other = home_smem[n], other_smem[n]
        block, tile = other >> 5, other & 31
        step_d = jnp.where(block < 3, -1, jnp.where(block < 6, 0, 1))
        step_p = block - 3 * (step_d + 1) - 1
        far = [near[block, c, pl.ds(tile, 1), :] for c in range(4)]
        far[0] = far[0] - period(step_d, dom)
        far[1] = far[1] - period(step_p, pen)
        rows = pair_push(jnp.concatenate(far, axis=0), against[home])
        for c in range(3):
            pushes[c, pl.ds(n, 1), :] = rows[c]
        return carry

    lax.fori_loop(0, PAIRS, pair, 0, unroll=4)
    tile_ids = lax.broadcasted_iota(jnp.int32, (TILES, PAIRS), 0)
    owners = jnp.where(home_vmem[...] == tile_ids, 1.0, 0.0).astype(bf16)
    for c in range(3):
        high, low = split(pushes[c])
        short_ref[c] = (dot(owners, high) + dot(owners, low)) * charge

    sent_3 = arrived(recv_d, 3, peer_one_a)
    pot_high, pot_low = split(from_z(taken(recv_d), picks[1536:]))
    for n in range(2):
        pot_parts[:128, 128 * n : 128 * n + 128] = pot_high
        pot_parts[128:, 128 * n : 128 * n + 128] = pot_low

    def interpolate(step, carry):
        for n in range(2):
            tile = step * 2 + n
            wide = dot(pot_parts[...], z_table[tile])
            along = wide[:128] + wide[128:]
            value = [along[8 * k : 8 * k + 8, :128] for k in range(16)]
            slope = [along[8 * k : 8 * k + 8, 128:] for k in range(16)]
            w_x, s_x, w_y, s_y = (xy_table[tile, 16 * k : 16 * k + 16] for k in range(4))
            by_y = [[], [], []]
            for y in range(SIDE):
                by_y[0].append(across(w_y, y) * value[y])
                by_y[1].append(across(s_y, y) * value[y])
                by_y[2].append(across(w_y, y) * slope[y])
            by_x = [[], [], []]
            for x in range(8, SIDE):
                by_x[0].append(across(s_x, x) * value[x + 3])
                by_x[1].append(across(w_x, x) * value[x + 3])
                by_x[2].append(across(w_x, x) * slope[x + 3])
            ends_x, ends_y = (s_x, w_x, w_x), (w_y, s_y, w_y)
            for c in range(3):
                total = ends_x[c][:8] * sum(by_y[c][1:], by_y[c][0])
                total += ends_y[c][:8] * sum(by_x[c][1:], by_x[c][0])
                own = slope if c == 2 else value
                corner = xy_table[tile, 64 + 16 * c : 80 + 16 * c]
                total += corner[:8] * own[14] + corner[8:] * own[15]
                grads[c, pl.ds(tile, 1), :] = jnp.sum(total, axis=0, keepdims=True)
        return carry

    lax.fori_loop(0, TILES // 2, interpolate, 0, unroll=4)
    for sent in (sent_0, sent_1, sent_2, sent_3):
        sent.wait_send()
    for c in range(3):
        long_ref[c] = grads[c] * charge


def on_device(atoms, pair_home, pair_other, *tables):
    hbm = pl.BlockSpec(memory_space=pl.ANY)
    vmem = pl.BlockSpec(memory_space=pltpu.VMEM)
    blocks = atoms.reshape(4, TILES, TILE)
    homes = pair_home.reshape(PAIRS)
    others = pair_other.reshape(PAIRS)
    force = jax.ShapeDtypeStruct((3, TILES, TILE), f32)
    message = pltpu.VMEM((PEERS, 4, NG), f32)
    short, long = pl.pallas_call(
        kernel,
        out_shape=(force, force),
        in_specs=[hbm] * (4 + len(NAMES)),
        out_specs=(vmem, vmem),
        scratch_shapes=[
            pltpu.SMEM((PAIRS,), jnp.int32),
            pltpu.SMEM((PAIRS,), jnp.int32),
            pltpu.VMEM((1, PAIRS), jnp.int32),
            pltpu.VMEM((9, 4, TILES, TILE), f32),
            pltpu.VMEM((FIELDS, TILES, TILE), f32),
            pltpu.VMEM((NG, NG), f32),
            pltpu.VMEM((3, PAIRS, TILE), f32),
            pltpu.VMEM((TILES, 16, 4 * TILE), bf16),
            pltpu.VMEM((3, TILES, TILE), f32),
            pltpu.VMEM((2 * NG, 2 * NG), bf16),
            pltpu.VMEM((TILES, 2 * NG, 2 * TILE), bf16),
            pltpu.VMEM((TILES, 112, TILE), f32),
            message,
            message,
            message,
            message,
            pltpu.VMEM((8, 4, NG), f32),
            message,
            message,
            message,
            *[pltpu.VMEM(t.shape, t.dtype) for t in tables],
            pltpu.SemaphoreType.DMA((len(NAMES) + 3,)),
            pltpu.SemaphoreType.DMA,
            pltpu.SemaphoreType.DMA((4,)),
            pltpu.SemaphoreType.DMA((4,)),
            pltpu.SemaphoreType.DMA((8,)),
            pltpu.SemaphoreType.DMA((8,)),
        ],
        compiler_params=pltpu.CompilerParams(
            collective_id=0, has_side_effects=True, vmem_limit_bytes=48 << 20
        ),
        name="forces",
    )(
        *(
            pltpu.with_memory_space_constraint(operand, pltpu.HBM)
            for operand in (blocks, homes, others, homes.reshape(1, PAIRS), *tables)
        )
    )
    total_atoms = 4 * 16 * 16 * TILES * TILE
    short = short * (32.0 * 2.0 / math.sqrt(256.0))
    long = long * (-0.4 * NG / math.sqrt(NG * total_atoms))
    return short.reshape(3, 1, 1, TILES * TILE), long.reshape(3, 1, 1, TILES * TILE)


def solution(mesh):
    tables = make_tables()

    def whole(atoms, pair_home, pair_other):
        fixed = [jnp.asarray(tables[name]) for name in NAMES]
        mapped = jax.shard_map(
            lambda a, h, o: on_device(a, h, o, *fixed),
            mesh=mesh,
            in_specs=(P(None, "grp", "dom", "pen"), P("grp", "dom", "pen"), P("grp", "dom", "pen")),
            out_specs=(P(None, "grp", "dom", "pen"), P(None, "grp", "dom", "pen")),
            check_vma=False,
        )
        return mapped(atoms, pair_home, pair_other)

    return whole
```
